32 devices in a mesh: dp: 4 (over y, core), seq: 8 (over z, x).
Axes of the slice: x: 2, y: 2, z: 4, core: 2. Of those that a mesh axis runs over, the one named last changes fastest.
Arguments:
- queries: bfloat16 [32, 2048, 512], P('dp', 'seq'), may hold values from -6 to 6
- enc_keys: bfloat16 [32, 2048, 512], P('dp', 'seq'), may hold values from -6 to 6
- enc_values: bfloat16 [32, 2048, 512], P('dp', 'seq'), may hold values from -6 to 6
- dec_ids: int32 [32, 2048], P('dp', 'seq'), may hold values from 0 to 15, never falling along the last dimension, each value on 1 to 512 neighbouring positions
- enc_ids: int32 [32, 2048], P('dp', 'seq'), may hold values from 0 to 15, never falling along the last dimension, each value on 1 to 512 neighbouring positions
Outputs:
- context: bfloat16 [32, 2048, 512], P('dp', 'seq')
The draws below stay inside these ranges and needn't reach their ends.
Inputs may be any that keep to these rules, and one draw needn't show every extreme that they name: `dec_ids`: along each row the numbers never fall; every number from 0 to 15 occurs in every row; a document holds 1 to 512 positions of a row, and some document holds exactly 512. `enc_ids`: along each row the numbers never fall; every number from 0 to 15 occurs in every row; a document holds 1 to 512 positions of a row, and some document holds exactly 512.
All inputs are finite; a program needn't handle non-finite values.
Results may differ from the reference program's by a relative error of at most 0.0047.
Values may be sent and summed in bfloat16 or wider, within the bound.
A program may use at most 128 MiB of HBM per device.

```python
import math
import jax
import jax.numpy as jnp
import numpy as np
from jax import lax

HEAD_DIM = 64
LEN = 2048
NDOC = 16
MOST = 512
HEADS = 8
INNER = 512
BATCH = 32


def draw_queries(key, part):
    base = jax.random.truncated_normal(jax.random.fold_in(key, 1), -6.0, 6.0, (BATCH, LEN, HEADS * HEAD_DIM), jnp.float32)
    result = 0.25 * base
    return result.astype(jnp.bfloat16)


def draw_enc_keys(key, part):
    base = jax.random.truncated_normal(jax.random.fold_in(key, 3), -6.0, 6.0, (BATCH, LEN, HEADS * HEAD_DIM), jnp.float32)
    result = base
    return result.astype(jnp.bfloat16)


def levels(rng, dims, cuts, least, top_value):
    level, own = 1.0, jax.random.fold_in(rng, 6)
    for dim, parts in cuts:
        heights = jnp.exp(jax.random.uniform(jax.random.fold_in(own, dim), (parts,), jnp.float32, least / len(cuts), top_value / len(cuts)))
        level = level * jnp.repeat(heights, dims[dim] // parts).reshape([-1 if axis == dim else 1 for axis in range(len(dims))])
    return level


def split_up(amount, total, most, lean):
    weights = [(1 << 20) // math.isqrt(grade ** lean) + 1 for grade in range(2, amount + 1)]
    surplus, given = total - most - (amount - 1), [1] * (amount - 1)
    while surplus > 0:
        free = [i for i in range(amount - 1) if given[i] < most]
        pool, left = sum([weights[i] for i in free]), surplus
        for i in free:
            addition = min(most - given[i], max(1, left * weights[i] // pool), surplus)
            given[i] = given[i] + addition
            surplus = surplus - addition
    return np.array([most] + given)


def uneven_parts(stream_key, number_of, total, most, slope):
    if number_of == 2:
        one = jax.random.randint(stream_key, (), max(1, total - most), min(most, total - 1) + 1)
        return jnp.stack([one, total - one])
    sizes = jnp.asarray(split_up(number_of, total, most, slope), jnp.int32)
    pairs = (number_of - 1) // 2
    giver, sink = sizes[1:1 + 2 * pairs:2], sizes[2:2 + 2 * pairs:2]
    slack = jnp.minimum(giver - 1, most - sink)
    moved = jax.random.randint(jax.random.fold_in(stream_key, 1), (pairs,), 0, 1 << 20) % (slack + 1)
    sizes = sizes.at[1:1 + 2 * pairs:2].set(giver - moved).at[2:2 + 2 * pairs:2].set(sink + moved)
    return sizes[jax.random.permutation(jax.random.fold_in(stream_key, 2), number_of)]


def scatter_about(key, extent, scale, reach, shards=(), kind=jnp.bfloat16):
    factor_of = levels(key, extent, shards, -0.22, 0.18) if shards else 1.0
    values = jax.random.normal(key, extent, jnp.float32) * scale * factor_of
    return jnp.minimum(jnp.maximum(values, -reach), reach).astype(kind)


def setup_inputs(seed: int = 0) -> dict:
    splits = jax.random.split(jax.random.key(seed), 6)
    return {
        "queries": draw_queries(jax.random.fold_in(splits[5], 71), 0),
        "enc_keys": draw_enc_keys(jax.random.fold_in(splits[5], 71), 0),
        "enc_values": scatter_about(splits[2], (BATCH, LEN, INNER), 1.0, 6.0, ((0, 4), (1, 8))),
        "dec_ids": jax.vmap(lambda own: jnp.searchsorted(jnp.cumsum(uneven_parts(own, NDOC, LEN, MOST, 2)), jnp.arange(LEN), side="right"))(jax.random.split(splits[3], BATCH)).reshape((BATCH, LEN)).astype(jnp.int32),
        "enc_ids": jax.vmap(lambda own: jnp.searchsorted(jnp.cumsum(uneven_parts(own, NDOC, LEN, MOST, 2)), jnp.arange(LEN), side="right"))(jax.random.split(splits[4], BATCH)).reshape((BATCH, LEN)).astype(jnp.int32),
    }


masked_score = -1.0e30


def attend_row(query_row, key_row, value_row, dec_row, enc_row):
    query_heads = query_row.astype(jnp.float32).reshape(LEN, HEADS, HEAD_DIM)
    key_heads = key_row.astype(jnp.float32).reshape(LEN, HEADS, HEAD_DIM)
    value_heads = value_row.astype(jnp.float32).reshape(LEN, HEADS, HEAD_DIM)
    query_span = min(512, LEN)
    pieces = []
    for offset in range(0, LEN, query_span):
        scores = jnp.einsum("qhd,khd->hqk", query_heads[offset:offset + query_span], key_heads,
                            precision=lax.Precision.HIGHEST)
        allowed = (dec_row[offset:offset + query_span][:, None] == enc_row[None, :])[None]
        scores = jnp.where(allowed, scores, masked_score)
        row_peak = jnp.max(scores, axis=2, keepdims=True)
        expos = jnp.where(allowed, jnp.exp(scores - row_peak), 0.0)
        row_total = jnp.sum(expos, axis=2, keepdims=True)
        weights = (expos / row_total).astype(jnp.bfloat16)
        weights = lax.optimization_barrier(weights).astype(jnp.float32)
        summed = jnp.einsum("hqk,khd->qhd", weights, value_heads, precision=lax.Precision.HIGHEST)
        pieces.append(summed.reshape(query_span, HEADS * HEAD_DIM).astype(jnp.bfloat16))
    return jnp.concatenate(pieces, axis=0)


def reference(queries, enc_keys, enc_values, dec_ids, enc_ids):
    def one_row(members):
        return attend_row(members[0], members[1], members[2], members[3], members[4])

    return lax.map(one_row, (queries, enc_keys, enc_values, dec_ids, enc_ids))
```

```python
import functools

import jax
import jax.numpy as jnp
from jax import lax
from jax.experimental import pallas as pl
from jax.experimental.pallas import tpu as pltpu
from jax.sharding import PartitionSpec as P

HEAD_DIM = 64
DOCS = 16
LANES = 128
SPAN = 256
PIECE = 32
PAD = 128
MASKED = -8192.0
SHARE = 7


def peer(me, shift, half):
    base = me // half * half
    return base + lax.rem(me - base + shift, half)


def greet(me, others):
    barrier = pltpu.get_barrier_semaphore()
    for target in others:
        pl.semaphore_signal(barrier, inc=1, device_id={"seq": target}, device_id_type=pl.DeviceIdType.MESH)
    pl.semaphore_wait(barrier, len(others))


def remote(src, dst, send_sem, recv_sem, target):
    return pltpu.make_async_remote_copy(
        src_ref=src,
        dst_ref=dst,
        send_sem=send_sem,
        recv_sem=recv_sem,
        device_id={"seq": target},
        device_id_type=pl.DeviceIdType.MESH,
    )


def gather_kernel(
    group, k_ref, dec_ref, enc_ref, v_ref, q_ref, k_out, dec_out, enc_out, v_out, q_out, held, ids_held, own_sem, ids_sem, send_sem, recv_sem, ids_send, ids_recv
):
    me = lax.axis_index("seq")
    half = group // 2
    width = k_out.shape[3]
    place = lax.rem(me, half)

    def columns(target):
        return k_ref.at[:, :, pl.ds(pl.multiple_of(lax.rem(target, half) * width, LANES), width)]

    def keys(shift):
        target = peer(me, shift, half)
        return remote(columns(target), k_out.at[place], send_sem.at[shift - 1], recv_sem.at[shift - 1], target)

    def ids(shift, slot, src, dst):
        at = slot * (group - 1) + shift - 1
        return remote(src, dst.at[me], ids_send.at[at], ids_recv.at[at], lax.rem(me + shift, group))

    both = ((0, dec_ref, dec_out), (1, enc_ref, enc_out))

    @pl.when(pl.program_id(0) == 0)
    def _():
        greet(me, [lax.rem(me + shift, group) for shift in range(1, group)])
        for shift in range(1, group):
            for slot, src, dst in both:
                ids(shift, slot, src, dst).start()
        for shift in range(half - 1, 0, -1):
            keys(shift).start()
        own = [pltpu.make_async_copy(columns(me), held, own_sem)]
        own += [pltpu.make_async_copy(src, ids_held.at[slot], ids_sem.at[slot]) for slot, src, _ in both]
        for copy in own:
            copy.start()
        for copy in own:
            copy.wait()
        own = [pltpu.make_async_copy(held, k_out.at[place], own_sem)]
        own += [pltpu.make_async_copy(ids_held.at[slot], dst.at[me], ids_sem.at[slot]) for slot, _, dst in both]
        for copy in own:
            copy.start()
        for copy in own:
            copy.wait()

    for src, dst in ((v_ref, v_out), (q_ref, q_out)):
        for target in range(half):
            dst[target, 0] = src[0, :, target * width : (target + 1) * width]

    @pl.when(pl.program_id(0) == pl.num_programs(0) - 1)
    def _():
        for shift in range(1, group):
            for slot, src, dst in both:
                ids(shift, slot, src, dst).wait()
        for shift in range(1, half):
            keys(shift).wait()


def gather(q, k, v, dec_ids, enc_ids, group):
    rows, count, features = k.shape
    half = group // 2
    width = features // half
    anywhere = pl.BlockSpec(memory_space=pl.ANY)
    block = pl.BlockSpec((1, count, features), lambda r: (r, 0, 0))
    packed = pl.BlockSpec((half, 1, count, width), lambda r: (0, r, 0, 0))
    spread = jax.ShapeDtypeStruct((half, rows, count, width), k.dtype)
    every = jax.ShapeDtypeStruct((group, rows, count), dec_ids.dtype)
    dma = pltpu.SemaphoreType.DMA
    return pl.pallas_call(
        functools.partial(gather_kernel, group),
        grid=(rows,),
        in_specs=[anywhere] * 3 + [block] * 2,
        out_specs=[anywhere] * 3 + [packed] * 2,
        out_shape=[spread, every, every, spread, spread],
        scratch_shapes=[
            pltpu.VMEM((rows, count, width), k.dtype),
            pltpu.VMEM((2, rows, count), dec_ids.dtype),
            dma,
            dma((2,)),
            dma((half - 1,)),
            dma((half - 1,)),
            dma((2 * (group - 1),)),
            dma((2 * (group - 1),)),
        ],
        compiler_params=pltpu.CompilerParams(collective_id=0, has_side_effects=True),
    )(k, dec_ids, enc_ids, v, q)


def give_back_kernel(group, o_ref, out_ref, held, own_sem, send_sem, recv_sem):
    me = lax.axis_index("seq")
    half = group // 2
    width = o_ref.shape[3]
    place = lax.rem(me, half)
    columns = out_ref.at[:, :, pl.ds(pl.multiple_of(place * width, LANES), width)]

    def transfer(shift):
        target = peer(me, shift, half)
        return remote(o_ref.at[lax.rem(target, half)], columns, send_sem.at[shift - 1], recv_sem.at[shift - 1], target)

    greet(me, [peer(me, shift, half) for shift in range(1, half)])
    for shift in range(half - 1, 0, -1):
        transfer(shift).start()
    own = pltpu.make_async_copy(o_ref.at[place], held, own_sem)
    own.start()
    own.wait()
    own = pltpu.make_async_copy(held, columns, own_sem)
    own.start()
    own.wait()
    for shift in range(1, half):
        transfer(shift).wait()


def give_back(o, group):
    half, rows, count, width = o.shape
    return pl.pallas_call(
        functools.partial(give_back_kernel, group),
        in_specs=[pl.BlockSpec(memory_space=pl.ANY)],
        out_specs=pl.BlockSpec(memory_space=pl.ANY),
        out_shape=jax.ShapeDtypeStruct((rows, count, half * width), o.dtype),
        scratch_shapes=[
            pltpu.VMEM((rows, count, width), o.dtype),
            pltpu.SemaphoreType.DMA,
            pltpu.SemaphoreType.DMA((half - 1,)),
            pltpu.SemaphoreType.DMA((half - 1,)),
        ],
        compiler_params=pltpu.CompilerParams(collective_id=1, has_side_effects=True),
    )(o)


def pack_kernel(table_ref, x_ref, o_ref):
    _, rows, count, width = x_ref.shape
    room = o_ref.shape[0]
    o_ref[...] = jnp.zeros(o_ref.shape, o_ref.dtype)
    for row in range(rows):
        offset, start, amount = table_ref[0, row], table_ref[1, row], table_ref[2, row]
        pieces = jnp.maximum(jnp.minimum(amount, room - PAD - offset), 0) // PIECE

        def move(index, carry):
            at = start + index * PIECE
            into = pl.multiple_of(offset + index * PIECE, PIECE)
            o_ref[pl.ds(into, PIECE), :] = x_ref[at // count, row, pl.ds(pl.multiple_of(at % count, PIECE), PIECE), :]
            return carry

        lax.fori_loop(0, pieces, move, 0)


def pack(table, x, room):
    half, rows, count, width = x.shape
    return pl.pallas_call(
        pack_kernel,
        grid_spec=pltpu.PrefetchScalarGridSpec(
            num_scalar_prefetch=1,
            grid=(1,),
            in_specs=[pl.BlockSpec(x.shape, lambda r, *_: (0, 0, 0, 0))],
            out_specs=pl.BlockSpec((room, width), lambda r, *_: (0, 0)),
        ),
        out_shape=jax.ShapeDtypeStruct((room, width), x.dtype),
        cost_estimate=pl.CostEstimate(flops=2000000, bytes_accessed=4 * x.size, transcendentals=0),
    )(table, x)


def attend_kernel(mode, table_ref, q_ref, k_ref, v_ref, dec_ref, enc_ref, *rest):
    if mode:
        more_k, more_v, before_ref, o_ref, keys, values = rest
    else:
        o_ref, keys, values = rest
    half, _, count, width = q_ref.shape
    length = half * count
    span = max(SPAN, count)
    slabs = span // count
    blocks = length // span
    heads = width // HEAD_DIM
    row = pl.program_id(0)
    first = table_ref[row, 3 * blocks + 1] * length

    def entry(kind, block):
        return table_ref[row, kind * blocks + block]

    wanted = [entry(2, block) == mode for block in range(blocks)]
    begin, end = jnp.int32(2 * length), jnp.int32(0)
    for block in range(blocks):
        low = entry(0, block)
        begin = jnp.where(wanted[block], jnp.minimum(begin, low), begin)
        end = jnp.where(wanted[block], jnp.maximum(end, low + entry(1, block) * span), end)

    def place(at, key, value):
        ids = enc_ref[0, :, pl.ds(at, LANES)]
        documents = lax.broadcasted_iota(jnp.int32, (LANES, LANES), 0)
        miss = jnp.where((documents == ids) | (documents >= DOCS), 0.0, MASKED).astype(jnp.bfloat16)
        keys[pl.ds(at, LANES), :width] = key
        keys[pl.ds(at, LANES), width:] = miss.T
        values[:, pl.ds(at, LANES)] = value.T

    chunk = min(LANES, count)

    def prepare(index, carry):
        at = pl.multiple_of(index * LANES, LANES)
        local = at - first
        mine = (local >= 0) & (local < length)

        @pl.when(mine)
        def _():
            if count >= LANES:
                slab = local // count
                inside = pl.ds(pl.multiple_of(local % count, LANES), LANES)
                place(at, k_ref[slab, 0, inside, :], v_ref[slab, 0, inside, :])
            else:
                slab = pl.ds(local // count, LANES // count)
                place(at, k_ref[slab, 0].reshape(LANES, width), v_ref[slab, 0].reshape(LANES, width))

        @pl.when(jnp.logical_not(mine))
        def _():
            if mode:
                room = more_k.shape[0]
                into = jnp.clip(table_ref[row, 3 * blocks] + at, 0, room - LANES)
                into = pl.ds(pl.multiple_of(into, PIECE), LANES)
                place(at, more_k[into, :], more_v[into, :])
            else:
                nothing = jnp.zeros((LANES, width), jnp.bfloat16)
                place(at, nothing, nothing)

        return carry

    lax.fori_loop(begin // LANES, end // LANES, prepare, 0)

    for block in range(blocks):
        slab = pl.ds(block * slabs, slabs)

        @pl.when(wanted[block])
        def _():
            query = q_ref[slab, 0].reshape(span, width)
            ids = dec_ref[0, :, pl.ds(block * span, span)]
            documents = lax.broadcasted_iota(jnp.int32, (LANES, span), 0)
            hot = jnp.where(documents == ids, 1.0, 0.0).astype(jnp.bfloat16).T
            owner = lax.broadcasted_iota(jnp.int32, (span, width), 1) // HEAD_DIM
            sides = [
                jnp.concatenate([jnp.where(owner == head, query, jnp.zeros_like(query)), hot], axis=1)
                for head in range(heads)
            ]
            low = entry(0, block)

            def step(index, held):
                start = pl.multiple_of(low + index * span, LANES)
                key = keys[pl.ds(start, span), :]
                result = []
                for head in range(heads):
                    peak, total, summed = held[head]
                    scores = lax.dot_general(
                        key, sides[head], (((1,), (1,)), ((), ())), preferred_element_type=jnp.float32
                    )
                    fresh = jnp.maximum(peak, jnp.max(scores, axis=0, keepdims=True))
                    scale = jnp.exp(peak - fresh)
                    expos = jnp.exp(scores - fresh)
                    total = total * scale + jnp.sum(expos, axis=0, keepdims=True)
                    value = values[head * HEAD_DIM : (head + 1) * HEAD_DIM, pl.ds(start, span)]
                    summed = summed * scale + jnp.dot(
                        value, expos.astype(jnp.bfloat16), preferred_element_type=jnp.float32
                    )
                    result.append((fresh, total, summed))
                return tuple(result)

            init = (
                jnp.full((1, span), 4 * MASKED, jnp.float32),
                jnp.zeros((1, span), jnp.float32),
                jnp.zeros((HEAD_DIM, span), jnp.float32),
            )
            done = lax.fori_loop(0, entry(1, block), step, (init,) * heads)
            whole = jnp.concatenate([summed / total for _, total, summed in done], axis=0)
            o_ref[slab, 0] = whole.T.astype(jnp.bfloat16).reshape(slabs, count, width)

        if mode:

            @pl.when(jnp.logical_not(wanted[block]))
            def _():
                o_ref[slab, 0] = before_ref[slab, 0]


def attend(mode, table, q, k, v, dec_rows, enc_rows, *more):
    half, rows, count, width = q.shape
    length = half * count
    row_block = pl.BlockSpec((half, 1, count, width), lambda r, *_: (0, r, 0, 0))
    specs = [row_block] * 3
    specs += [pl.BlockSpec((1, 1, length), lambda r, *_: (r, 0, 0))]
    specs += [pl.BlockSpec((1, 1, 2 * length), lambda r, *_: (r, 0, 0))]
    if mode:
        specs += [pl.BlockSpec(more[0].shape, lambda r, *_: (0, 0))] * 2 + [row_block]
    return pl.pallas_call(
        functools.partial(attend_kernel, mode),
        grid_spec=pltpu.PrefetchScalarGridSpec(
            num_scalar_prefetch=1,
            grid=(rows,),
            in_specs=specs,
            out_specs=row_block,
            scratch_shapes=[
                pltpu.VMEM((2 * length, width + LANES), jnp.bfloat16),
                pltpu.VMEM((width, 2 * length), jnp.bfloat16),
            ],
        ),
        out_shape=jax.ShapeDtypeStruct(q.shape, q.dtype),
        cost_estimate=pl.CostEstimate(
            flops=rows * width // HEAD_DIM * length * length * 128,
            bytes_accessed=8 * rows * width * length,
            transcendentals=rows * length * length // 4,
        ),
    )(table, q, k, v, dec_rows, enc_rows, *more)


def tables(dec_rows, enc_rows, side):
    rows, whole = dec_rows.shape
    length = whole // 2
    mine = lax.dynamic_slice(dec_rows, (0, side * length), (rows, length))
    blocks = length // SPAN
    docs = mine.reshape(rows, blocks, SPAN)
    starts = jnp.concatenate([docs[:, :, 0], dec_rows[:, length : length + 1]], axis=1)
    ends = jnp.concatenate([docs[:, :, -1], dec_rows[:, length - 1 : length]], axis=1)
    before = jnp.sum(enc_rows[:, None, :] < starts[:, :, None], axis=2, dtype=jnp.int32)
    upto = jnp.sum(enc_rows[:, None, :] <= ends[:, :, None], axis=2, dtype=jnp.int32)
    up = jnp.maximum(length - before[:, blocks], 0)
    down = jnp.maximum(upto[:, blocks] - length, 0)
    up, down = (-(-amount // PIECE) * PIECE for amount in (up, down))
    before, upto = before[:, :blocks], upto[:, :blocks]
    crosses = jnp.where(side == 0, upto > length, before < length).astype(jnp.int32)
    low = before // LANES * LANES
    steps = (upto - low + SPAN - 1) // SPAN
    low = jnp.minimum(low, whole - steps * SPAN)
    sent, got = jnp.where(side == 0, up, down), jnp.where(side == 0, down, up)
    offset_of = [PAD + jnp.cumsum(amount) - amount for amount in (sent, got)]
    first = jnp.where(side == 0, length - sent, 0)
    send = jnp.stack([offset_of[0], first, sent])
    base = offset_of[1] - jnp.where(side == 0, length, length - got)
    known = jnp.concatenate([low, steps, crosses, base[:, None], jnp.full((rows, 1), side, jnp.int32)], axis=1)
    return send, known, mine, jnp.maximum(jnp.sum(up), jnp.sum(down))


def local(queries, enc_keys, enc_values, dec_ids, enc_ids):
    group = lax.axis_size("seq")
    half = group // 2
    rows, count, features = queries.shape
    length = half * count
    side = lax.axis_index("seq") // half
    k, dec_all, enc_all, v_packed, q_packed = gather(queries, enc_keys, enc_values, dec_ids, enc_ids, group)
    sides = [list(range(half)), list(range(half, group))]

    def exchange(block):
        return lax.all_to_all(block, "seq", split_axis=0, concat_axis=0, axis_index_groups=sides, tiled=True)

    def cross(block):
        return lax.ppermute(block, "seq", [(i, (i + half) % group) for i in range(group)])

    v = exchange(v_packed)
    q = exchange(q_packed)
    dec_rows, enc_rows = (x.transpose(1, 0, 2).reshape(rows, 2 * length) for x in (dec_all, enc_all))
    send, known, mine, most = tables(dec_rows, enc_rows, side)
    most = lax.pmax(most, "dp")
    room = rows * length * SHARE // 16 // 128 * 128 + 2 * PAD
    full = rows * length + 2 * PAD
    more_k = cross(pack(send, k, room))
    more_v = cross(pack(send, v, room))
    mine, enc_rows = mine[:, None, :], enc_rows[:, None, :]
    early = attend(0, known, q, k, v, mine, enc_rows)

    def enough(more_k, more_v):
        return attend(1, known, q, k, v, mine, enc_rows, more_k, more_v, early)

    def overflow(more_k, more_v):
        more_k, more_v = cross(pack(send, k, full)), cross(pack(send, v, full))
        return attend(1, known, q, k, v, mine, enc_rows, more_k, more_v, early)

    return give_back(lax.cond(most <= room - 2 * PAD, enough, overflow, more_k, more_v), group)


def solution(mesh):
    in_specs = (
        P("dp", "seq", None),
        P("dp", "seq", None),
        P("dp", "seq", None),
        P("dp", "seq"),
        P("dp", "seq"),
    )
    out_specs = P("dp", "seq", None)
    return jax.shard_map(local, mesh=mesh, in_specs=in_specs, out_specs=out_specs, check_vma=False)
```

```python
import functools

import jax
import jax.numpy as jnp
from jax import lax
from jax.experimental import pallas as pl
from jax.experimental.pallas import tpu as pltpu
from jax.sharding import PartitionSpec as P


HEAD_DIM = 64
DOCS = 16
LANES = 128
SPAN = 256
STRIDE = 512
PIECE = 32
PAD = 128
MASKED = -8192.0
SHARE = 7


def peer(me, shift, half):
    base = me // half * half
    return base + lax.rem(me - base + shift, half)


def greet(others):
    barrier = pltpu.get_barrier_semaphore()
    for target in others:
        pl.semaphore_signal(barrier, inc=1, device_id={"seq": target}, device_id_type=pl.DeviceIdType.MESH)
    pl.semaphore_wait(barrier, len(others))


def remote(src, dst, send_sem, recv_sem, target):
    return pltpu.make_async_remote_copy(
        src_ref=src,
        dst_ref=dst,
        send_sem=send_sem,
        recv_sem=recv_sem,
        device_id={"seq": target},
        device_id_type=pl.DeviceIdType.MESH,
    )


def gather_kernel(
    group, k_ref, dec_ref, enc_ref, v_ref, q_ref, k_out, dec_out, enc_out, v_out, q_out, held, ids_held, own_sem, ids_sem, send_sem, recv_sem, ids_send, ids_recv
):
    me = lax.axis_index("seq")
    half = group // 2
    width = k_out.shape[3]
    place = lax.rem(me, half)

    def columns(target):
        return k_ref.at[:, :, pl.ds(pl.multiple_of(lax.rem(target, half) * width, LANES), width)]

    def keys(shift):
        target = peer(me, shift, half)
        return remote(columns(target), k_out.at[place], send_sem.at[shift - 1], recv_sem.at[shift - 1], target)

    def ids(shift, slot, src, dst):
        at = slot * (group - 1) + shift - 1
        return remote(src, dst.at[me], ids_send.at[at], ids_recv.at[at], lax.rem(me + shift, group))

    both = ((0, dec_ref, dec_out), (1, enc_ref, enc_out))

    @pl.when(pl.program_id(0) == 0)
    def _():
        greet([lax.rem(me + shift, group) for shift in range(1, group)])
        for shift in range(1, group):
            for slot, src, dst in both:
                ids(shift, slot, src, dst).start()
        for shift in range(half - 1, 0, -1):
            keys(shift).start()
        own = [pltpu.make_async_copy(columns(me), held, own_sem)]
        own += [pltpu.make_async_copy(src, ids_held.at[slot], ids_sem.at[slot]) for slot, src, _ in both]
        for copy in own:
            copy.start()
        for copy in own:
            copy.wait()
        own = [pltpu.make_async_copy(held, k_out.at[place], own_sem)]
        own += [pltpu.make_async_copy(ids_held.at[slot], dst.at[me], ids_sem.at[slot]) for slot, _, dst in both]
        for copy in own:
            copy.start()
        for copy in own:
            copy.wait()

    for src, dst in ((v_ref, v_out), (q_ref, q_out)):
        for target in range(half):
            dst[target, 0] = src[0, :, target * width : (target + 1) * width]

    @pl.when(pl.program_id(0) == pl.num_programs(0) - 1)
    def _():
        for shift in range(1, group):
            for slot, src, dst in both:
                ids(shift, slot, src, dst).wait()
        for shift in range(1, half):
            keys(shift).wait()


def gather(q, k, v, dec_ids, enc_ids, group):
    rows, count, features = k.shape
    half = group // 2
    width = features // half
    anywhere = pl.BlockSpec(memory_space=pl.ANY)
    block = pl.BlockSpec((1, count, features), lambda r: (r, 0, 0))
    packed = pl.BlockSpec((half, 1, count, width), lambda r: (0, r, 0, 0))
    spread = jax.ShapeDtypeStruct((half, rows, count, width), k.dtype)
    every = jax.ShapeDtypeStruct((group, rows, count), dec_ids.dtype)
    dma = pltpu.SemaphoreType.DMA
    return pl.pallas_call(
        functools.partial(gather_kernel, group),
        grid=(rows,),
        in_specs=[anywhere] * 3 + [block] * 2,
        out_specs=[anywhere] * 3 + [packed] * 2,
        out_shape=[spread, every, every, spread, spread],
        scratch_shapes=[
            pltpu.VMEM((rows, count, width), k.dtype),
            pltpu.VMEM((2, rows, count), dec_ids.dtype),
            dma,
            dma((2,)),
            dma((half - 1,)),
            dma((half - 1,)),
            dma((2 * (group - 1),)),
            dma((2 * (group - 1),)),
        ],
        compiler_params=pltpu.CompilerParams(collective_id=0, has_side_effects=True),
    )(k, dec_ids, enc_ids, v, q)


def give_back_kernel(group, o_ref, out_ref, held, own_sem, send_sem, recv_sem):
    me = lax.axis_index("seq")
    half = group // 2
    width = o_ref.shape[3]
    place = lax.rem(me, half)
    columns = out_ref.at[:, :, pl.ds(pl.multiple_of(place * width, LANES), width)]

    def transfer(shift):
        target = peer(me, shift, half)
        return remote(o_ref.at[lax.rem(target, half)], columns, send_sem.at[shift - 1], recv_sem.at[shift - 1], target)

    greet([peer(me, shift, half) for shift in range(1, half)])
    for shift in range(half - 1, 0, -1):
        transfer(shift).start()
    own = pltpu.make_async_copy(o_ref.at[place], held, own_sem)
    own.start()
    own.wait()
    own = pltpu.make_async_copy(held, columns, own_sem)
    own.start()
    own.wait()
    for shift in range(1, half):
        transfer(shift).wait()


def give_back(o, group):
    half, rows, count, width = o.shape
    return pl.pallas_call(
        functools.partial(give_back_kernel, group),
        in_specs=[pl.BlockSpec(memory_space=pl.ANY)],
        out_specs=pl.BlockSpec(memory_space=pl.ANY),
        out_shape=jax.ShapeDtypeStruct((rows, count, half * width), o.dtype),
        scratch_shapes=[
            pltpu.VMEM((rows, count, width), o.dtype),
            pltpu.SemaphoreType.DMA,
            pltpu.SemaphoreType.DMA((half - 1,)),
            pltpu.SemaphoreType.DMA((half - 1,)),
        ],
        compiler_params=pltpu.CompilerParams(collective_id=1, has_side_effects=True),
    )(o)


def pack_kernel(table_ref, x_ref, o_ref):
    _, rows, count, _ = x_ref.shape
    room = o_ref.shape[0]
    o_ref[...] = jnp.zeros(o_ref.shape, o_ref.dtype)
    for row in range(rows):
        offset, start, amount = table_ref[0, row], table_ref[1, row], table_ref[2, row]
        pieces = jnp.maximum(jnp.minimum(amount, room - PAD - offset), 0) // PIECE

        def move(index, carry):
            at = start + index * PIECE
            into = pl.multiple_of(offset + index * PIECE, PIECE)
            o_ref[pl.ds(into, PIECE), :] = x_ref[at // count, row, pl.ds(pl.multiple_of(at % count, PIECE), PIECE), :]
            return carry

        lax.fori_loop(0, pieces, move, 0)


def pack(table, x, room):
    _, _, _, width = x.shape
    return pl.pallas_call(
        pack_kernel,
        grid_spec=pltpu.PrefetchScalarGridSpec(
            num_scalar_prefetch=1,
            grid=(1,),
            in_specs=[pl.BlockSpec(x.shape, lambda r, *_: (0, 0, 0, 0))],
            out_specs=pl.BlockSpec((room, width), lambda r, *_: (0, 0)),
        ),
        out_shape=jax.ShapeDtypeStruct((room, width), x.dtype),
        cost_estimate=pl.CostEstimate(flops=2000000, bytes_accessed=4 * x.size, transcendentals=0),
    )(table, x)


def attend_kernel(mode, table_ref, q_ref, k_ref, v_ref, bounds_ref, *rest):
    if mode:
        more_k, more_v, before_ref, o_ref, keys, values = rest
    else:
        o_ref, keys, values = rest
    half, _, count, width = q_ref.shape
    length = half * count
    span = max(SPAN, count)
    stride = min(STRIDE, length)
    slabs = span // count
    blocks = length // span
    heads = width // HEAD_DIM
    row = pl.program_id(0)
    first = table_ref[row, 3 * blocks + 1] * length

    def entry(kind, block):
        return table_ref[row, kind * blocks + block]

    wanted = [entry(2, block) == mode for block in range(blocks)]
    begin, end = jnp.int32(2 * length), jnp.int32(0)
    for block in range(blocks):
        low = entry(0, block)
        begin = jnp.where(wanted[block], jnp.minimum(begin, low), begin)
        end = jnp.where(wanted[block], jnp.maximum(end, low + entry(1, block) * stride), end)

    def within(which, at, amount):
        position = at + lax.broadcasted_iota(jnp.int32, (amount, LANES), 0)
        return (position >= bounds_ref[0, which : which + 1]) & (position < bounds_ref[0, which + 1 : which + 2])

    def place(at, key, value):
        documents = lax.broadcasted_iota(jnp.int32, (LANES, LANES), 1)
        keys[pl.ds(at, LANES), :width] = key
        miss = jnp.where(within(0, at, LANES) | (documents >= DOCS), 0.0, MASKED)
        keys[pl.ds(at, LANES), width:] = miss.astype(jnp.bfloat16)
        values[:, pl.ds(at, LANES)] = value.T

    def prepare(index, carry):
        at = pl.multiple_of(index * LANES, LANES)
        local = at - first
        mine = (local >= 0) & (local < length)

        @pl.when(mine)
        def _():
            if count >= LANES:
                slab = local // count
                inside = pl.ds(pl.multiple_of(local % count, LANES), LANES)
                place(at, k_ref[slab, 0, inside, :], v_ref[slab, 0, inside, :])
            else:
                slab = pl.ds(local // count, LANES // count)
                place(at, k_ref[slab, 0].reshape(LANES, width), v_ref[slab, 0].reshape(LANES, width))

        @pl.when(jnp.logical_not(mine))
        def _():
            if mode:
                room = more_k.shape[0]
                into = jnp.clip(table_ref[row, 3 * blocks] + at, 0, room - LANES)
                into = pl.ds(pl.multiple_of(into, PIECE), LANES)
                place(at, more_k[into, :], more_v[into, :])
            else:
                nothing = jnp.zeros((LANES, width), jnp.bfloat16)
                place(at, nothing, nothing)

        return carry

    lax.fori_loop(begin // LANES, end // LANES, prepare, 0)

    for block in range(blocks):
        slab = pl.ds(block * slabs, slabs)

        @pl.when(wanted[block])
        def _():
            query = q_ref[slab, 0].reshape(span, width)
            hot = jnp.where(within(2, first + block * span, span), 1.0, 0.0).astype(jnp.bfloat16)
            owner = lax.broadcasted_iota(jnp.int32, (span, width), 1) // HEAD_DIM
            sides = [
                jnp.concatenate([jnp.where(owner == head, query, jnp.zeros_like(query)), hot], axis=1)
                for head in range(heads)
            ]
            low = entry(0, block)

            def step(index, held):
                start = pl.multiple_of(low + index * stride, LANES)
                key = keys[pl.ds(start, stride), :]
                result = []
                for head in range(heads):
                    peak, total, summed = held[head]
                    scores = lax.dot_general(
                        key, sides[head], (((1,), (1,)), ((), ())), preferred_element_type=jnp.float32
                    )
                    fresh = jnp.maximum(peak, jnp.max(scores, axis=0, keepdims=True))
                    scale = jnp.exp(peak - fresh)
                    expos = jnp.exp(scores - fresh)
                    total = total * scale + jnp.sum(expos, axis=0, keepdims=True)
                    value = values[head * HEAD_DIM : (head + 1) * HEAD_DIM, pl.ds(start, stride)]
                    summed = summed * scale + jnp.dot(
                        value, expos.astype(jnp.bfloat16), preferred_element_type=jnp.float32
                    )
                    result.append((fresh, total, summed))
                return tuple(result)

            init = (
                jnp.full((1, span), 4 * MASKED, jnp.float32),
                jnp.zeros((1, span), jnp.float32),
                jnp.zeros((HEAD_DIM, span), jnp.float32),
            )
            done = lax.fori_loop(0, entry(1, block), step, (init,) * heads)
            whole = jnp.concatenate([summed / total for _, total, summed in done], axis=0)
            o_ref[slab, 0] = whole.T.astype(jnp.bfloat16).reshape(slabs, count, width)

        if mode:

            @pl.when(jnp.logical_not(wanted[block]))
            def _():
                o_ref[slab, 0] = before_ref[slab, 0]


def attend(mode, table, q, k, v, bounds, *more):
    half, rows, count, width = q.shape
    length = half * count
    row_block = pl.BlockSpec((half, 1, count, width), lambda r, *_: (0, r, 0, 0))
    specs = [row_block] * 3
    specs += [pl.BlockSpec((1, *bounds.shape[1:]), lambda r, *_: (r, 0, 0))]
    if mode:
        specs += [pl.BlockSpec(more[0].shape, lambda r, *_: (0, 0))] * 2 + [row_block]
    return pl.pallas_call(
        functools.partial(attend_kernel, mode),
        grid_spec=pltpu.PrefetchScalarGridSpec(
            num_scalar_prefetch=1,
            grid=(rows,),
            in_specs=specs,
            out_specs=row_block,
            scratch_shapes=[
                pltpu.VMEM((2 * length, width + LANES), jnp.bfloat16),
                pltpu.VMEM((width, 2 * length), jnp.bfloat16),
            ],
        ),
        out_shape=jax.ShapeDtypeStruct(q.shape, q.dtype),
        cost_estimate=pl.CostEstimate(
            flops=rows * width // HEAD_DIM * length * length * 128,
            bytes_accessed=8 * rows * width * length,
            transcendentals=rows * length * length // 4,
        ),
    )(table, q, k, v, bounds, *more)


def tables(dec_rows, enc_rows, side):
    rows, whole = dec_rows.shape
    length = whole // 2
    blocks = length // SPAN
    stride = min(STRIDE, length)
    numbers = jnp.arange(LANES, dtype=jnp.int32)[None, :, None]
    bounds = []
    for ids in (enc_rows, dec_rows):
        bounds += [jnp.sum(ids[:, None, :] < numbers, axis=2), jnp.sum(ids[:, None, :] <= numbers, axis=2)]
    bounds = jnp.stack(bounds, axis=1).astype(jnp.int32)
    mine = lax.dynamic_slice(dec_rows, (0, side * length), (rows, length))
    docs = mine.reshape(rows, blocks, SPAN)
    starts = jnp.concatenate([docs[:, :, 0], dec_rows[:, length : length + 1]], axis=1)
    ends = jnp.concatenate([docs[:, :, -1], dec_rows[:, length - 1 : length]], axis=1)
    before = jnp.sum(enc_rows[:, None, :] < starts[:, :, None], axis=2, dtype=jnp.int32)
    upto = jnp.sum(enc_rows[:, None, :] <= ends[:, :, None], axis=2, dtype=jnp.int32)
    up = jnp.maximum(length - before[:, blocks], 0)
    down = jnp.maximum(upto[:, blocks] - length, 0)
    up, down = (-(-amount // PIECE) * PIECE for amount in (up, down))
    before, upto = before[:, :blocks], upto[:, :blocks]
    crosses = jnp.where(side == 0, upto > length, before < length).astype(jnp.int32)
    low = before // LANES * LANES
    steps = (upto - low + stride - 1) // stride
    low = jnp.minimum(low, whole - steps * stride)
    sent, got = jnp.where(side == 0, up, down), jnp.where(side == 0, down, up)
    offset_of = [PAD + jnp.cumsum(amount) - amount for amount in (sent, got)]
    first = jnp.where(side == 0, length - sent, 0)
    send = jnp.stack([offset_of[0], first, sent])
    base = offset_of[1] - jnp.where(side == 0, length, length - got)
    known = jnp.concatenate([low, steps, crosses, base[:, None], jnp.full((rows, 1), side, jnp.int32)], axis=1)
    return send, known, bounds, jnp.maximum(jnp.sum(up), jnp.sum(down))


def whole(queries, enc_keys, enc_values, dec_ids, enc_ids):
    group = lax.axis_size("seq")
    half = group // 2
    rows, count, _ = queries.shape
    length = half * count
    side = lax.axis_index("seq") // half
    k, dec_all, enc_all, v_packed, q_packed = gather(queries, enc_keys, enc_values, dec_ids, enc_ids, group)
    sides = [list(range(half)), list(range(half, group))]

    def exchange(block):
        return lax.all_to_all(block, "seq", split_axis=0, concat_axis=0, axis_index_groups=sides, tiled=True)

    def cross(block):
        return lax.ppermute(block, "seq", [(i, (i + half) % group) for i in range(group)])

    dec_rows, enc_rows = (x.transpose(1, 0, 2).reshape(rows, 2 * length) for x in (dec_all, enc_all))
    send, known, bounds, most = tables(dec_rows, enc_rows, side)
    room = rows * length * SHARE // 16 // 128 * 128 + 2 * PAD
    full = rows * length + 2 * PAD
    k_packed, v_packed = lax.optimization_barrier((pack(send, k, room), v_packed))
    more_k = cross(k_packed)
    v = exchange(v_packed)
    v_cross, q_packed = lax.optimization_barrier((pack(send, v, room), q_packed))
    more_v = cross(v_cross)
    q = exchange(q_packed)
    most = lax.pmax(most, "dp")
    early = attend(0, known, q, k, v, bounds)

    def enough(more_k, more_v):
        return attend(1, known, q, k, v, bounds, more_k, more_v, early)

    def overflow(more_k, more_v):
        more_k, more_v = cross(pack(send, k, full)), cross(pack(send, v, full))
        return attend(1, known, q, k, v, bounds, more_k, more_v, early)

    return give_back(lax.cond(most <= room - 2 * PAD, enough, overflow, more_k, more_v), group)


def solution(mesh):
    in_specs = (
        P("dp", "seq", None),
        P("dp", "seq", None),
        P("dp", "seq", None),
        P("dp", "seq"),
        P("dp", "seq"),
    )
    out_specs = P("dp", "seq", None)
    return jax.shard_map(whole, mesh=mesh, in_specs=in_specs, out_specs=out_specs, check_vma=False)
```

```python
import functools

import jax
import jax.numpy as jnp
from jax import lax
from jax.experimental import pallas as pl
from jax.experimental.pallas import tpu as pltpu
from jax.sharding import PartitionSpec as P


HEAD_DIM = 64
DOCS = 16
LANES = 128
SPAN = 256
STRIDE = 512
PIECE = 32
PAD = 128
MASKED = -8192.0
ROOM = 11
TRIP = 512


def peer(me, shift, half):
    base = me // half * half
    return base + lax.rem(me - base + shift, half)


def greet(others):
    barrier = pltpu.get_barrier_semaphore()
    for target in others:
        pl.semaphore_signal(barrier, inc=1, device_id={"seq": target}, device_id_type=pl.DeviceIdType.MESH)
    pl.semaphore_wait(barrier, len(others))


def remote(src, dst, send_sem, recv_sem, target):
    return pltpu.make_async_remote_copy(
        src_ref=src,
        dst_ref=dst,
        send_sem=send_sem,
        recv_sem=recv_sem,
        device_id={"seq": target},
        device_id_type=pl.DeviceIdType.MESH,
    )


def gather_kernel(
    group, k_ref, v_ref, dec_ref, enc_ref, q_ref, k_out, v_out, dec_out, enc_out, q_out, held, ids_held, own_sem, ids_sem, send_sem, recv_sem, ids_send, ids_recv
):
    me = lax.axis_index("seq")
    half = group // 2
    width = k_out.shape[3]
    place = lax.rem(me, half)
    large = ((0, k_ref, k_out), (1, v_ref, v_out))
    small = ((0, dec_ref, dec_out), (1, enc_ref, enc_out))

    def columns(src, target):
        return src.at[:, :, pl.ds(pl.multiple_of(lax.rem(target, half) * width, LANES), width)]

    def heads(shift, slot, src, dst):
        target = peer(me, shift, half)
        at = slot * (half - 1) + shift - 1
        return remote(columns(src, target), dst.at[place], send_sem.at[at], recv_sem.at[at], target)

    def ids(shift, slot, src, dst):
        at = slot * (group - 1) + shift - 1
        return remote(src, dst.at[me], ids_send.at[at], ids_recv.at[at], lax.rem(me + shift, group))

    @pl.when(pl.program_id(0) == 0)
    def _():
        greet([lax.rem(me + shift, group) for shift in range(1, group)])
        for shift in range(1, group):
            for each in small:
                ids(shift, *each).start()
        for each in large:
            for shift in range(half - 1, 0, -1):
                heads(shift, *each).start()
        own = [pltpu.make_async_copy(columns(src, me), held.at[slot], own_sem.at[slot]) for slot, src, _ in large]
        own += [pltpu.make_async_copy(src, ids_held.at[slot], ids_sem.at[slot]) for slot, src, _ in small]
        for copy in own:
            copy.start()
        for copy in own:
            copy.wait()
        own = [pltpu.make_async_copy(held.at[slot], dst.at[place], own_sem.at[slot]) for slot, _, dst in large]
        own += [pltpu.make_async_copy(ids_held.at[slot], dst.at[me], ids_sem.at[slot]) for slot, _, dst in small]
        for copy in own:
            copy.start()
        for copy in own:
            copy.wait()

    for target in range(half):
        q_out[target, 0] = q_ref[0, :, target * width : (target + 1) * width]

    @pl.when(pl.program_id(0) == pl.num_programs(0) - 1)
    def _():
        for shift in range(1, group):
            for each in small:
                ids(shift, *each).wait()
        for each in large:
            for shift in range(1, half):
                heads(shift, *each).wait()


def gather(q, k, v, dec_ids, enc_ids, group):
    rows, count, features = k.shape
    half = group // 2
    width = features // half
    anywhere = pl.BlockSpec(memory_space=pl.ANY)
    block = pl.BlockSpec((1, count, features), lambda r: (r, 0, 0))
    packed = pl.BlockSpec((half, 1, count, width), lambda r: (0, r, 0, 0))
    spread = jax.ShapeDtypeStruct((half, rows, count, width), k.dtype)
    every = jax.ShapeDtypeStruct((group, rows, count), dec_ids.dtype)
    dma = pltpu.SemaphoreType.DMA
    return pl.pallas_call(
        functools.partial(gather_kernel, group),
        grid=(rows,),
        in_specs=[anywhere] * 4 + [block],
        out_specs=[anywhere] * 4 + [packed],
        out_shape=[spread, spread, every, every, spread],
        scratch_shapes=[
            pltpu.VMEM((2, rows, count, width), k.dtype),
            pltpu.VMEM((2, rows, count), dec_ids.dtype),
            dma((2,)),
            dma((2,)),
            dma((2 * (half - 1),)),
            dma((2 * (half - 1),)),
            dma((2 * (group - 1),)),
            dma((2 * (group - 1),)),
        ],
        compiler_params=pltpu.CompilerParams(collective_id=0, has_side_effects=True),
    )(k, v, dec_ids, enc_ids, q)


def give_back_kernel(group, o_ref, out_ref, held, own_sem, send_sem, recv_sem):
    me = lax.axis_index("seq")
    half = group // 2
    width = o_ref.shape[3]
    place = lax.rem(me, half)
    columns = out_ref.at[:, :, pl.ds(pl.multiple_of(place * width, LANES), width)]

    def transfer(shift):
        target = peer(me, shift, half)
        return remote(o_ref.at[lax.rem(target, half)], columns, send_sem.at[shift - 1], recv_sem.at[shift - 1], target)

    greet([peer(me, shift, half) for shift in range(1, half)])
    for shift in range(half - 1, 0, -1):
        transfer(shift).start()
    own = pltpu.make_async_copy(o_ref.at[place], held, own_sem)
    own.start()
    own.wait()
    own = pltpu.make_async_copy(held, columns, own_sem)
    own.start()
    own.wait()
    for shift in range(1, half):
        transfer(shift).wait()


def give_back(o, group):
    half, rows, count, width = o.shape
    return pl.pallas_call(
        functools.partial(give_back_kernel, group),
        in_specs=[pl.BlockSpec(memory_space=pl.ANY)],
        out_specs=pl.BlockSpec(memory_space=pl.ANY),
        out_shape=jax.ShapeDtypeStruct((rows, count, half * width), o.dtype),
        scratch_shapes=[
            pltpu.VMEM((rows, count, width), o.dtype),
            pltpu.SemaphoreType.DMA,
            pltpu.SemaphoreType.DMA((half - 1,)),
            pltpu.SemaphoreType.DMA((half - 1,)),
        ],
        compiler_params=pltpu.CompilerParams(collective_id=1, has_side_effects=True),
    )(o)


def pack_kernel(table_ref, k_ref, v_ref, o_ref, rest_ref, stage):
    _, rows, count, width = k_ref.shape
    room = o_ref.shape[0]
    stage[...] = jnp.zeros(stage.shape, stage.dtype)
    for row in range(rows):
        offset, start, amount = table_ref[0, row], table_ref[1, row], table_ref[2, row]

        def move(index, carry):
            at = start + index * PIECE
            slab, inside = at // count, pl.ds(pl.multiple_of(at % count, PIECE), PIECE)
            into = pl.ds(pl.multiple_of(offset + index * PIECE, PIECE), PIECE)
            stage[into, :width] = k_ref[slab, row, inside, :]
            stage[into, width:] = v_ref[slab, row, inside, :]
            return carry

        lax.fori_loop(0, amount // PIECE, move, 0)
    o_ref[...] = stage[:room]
    rest_ref[...] = stage[room:]


def pack(table, k, v, room):
    half, rows, count, width = k.shape
    full = rows * half * count + 2 * PAD
    whole = pl.BlockSpec(k.shape, lambda r, *_: (0, 0, 0, 0))
    shapes = [(room, 2 * width), (full - room, 2 * width)]
    return pl.pallas_call(
        pack_kernel,
        grid_spec=pltpu.PrefetchScalarGridSpec(
            num_scalar_prefetch=1,
            grid=(1,),
            in_specs=[whole] * 2,
            out_specs=[pl.BlockSpec(shape, lambda r, *_: (0, 0)) for shape in shapes],
            scratch_shapes=[pltpu.VMEM((full, 2 * width), k.dtype)],
        ),
        out_shape=[jax.ShapeDtypeStruct(shape, k.dtype) for shape in shapes],
        cost_estimate=pl.CostEstimate(flops=2000000, bytes_accessed=8 * k.size, transcendentals=0),
    )(table, k, v)


def within(bounds_ref, which, at, amount):
    position = at + lax.broadcasted_iota(jnp.int32, (amount, LANES), 0)
    return (position >= bounds_ref[0, which : which + 1]) & (position < bounds_ref[0, which + 1 : which + 2])


def missing(bounds_ref, at, amount):
    documents = lax.broadcasted_iota(jnp.int32, (amount, LANES), 1)
    inside = within(bounds_ref, 0, at, amount) | (documents >= DOCS)
    return jnp.where(inside, 0.0, MASKED).astype(jnp.bfloat16)


def prepare_kernel(table_ref, k_ref, v_ref, bounds_ref, keys, values):
    half, _, count, width = k_ref.shape
    length = half * count
    keys[0, :, :width] = k_ref[:, 0].reshape(length, width)
    keys[0, :, width:] = missing(bounds_ref, table_ref[0, table_ref.shape[1] - 1] * length, length)
    values[0] = v_ref[:, 0].reshape(length, width).T


def prepare(table, k, v, bounds):
    half, rows, count, width = k.shape
    length = half * count
    row_block = pl.BlockSpec((half, 1, count, width), lambda r, *_: (0, r, 0, 0))
    shapes = [(1, length, width + LANES), (1, width, length)]
    return pl.pallas_call(
        prepare_kernel,
        grid_spec=pltpu.PrefetchScalarGridSpec(
            num_scalar_prefetch=1,
            grid=(rows,),
            in_specs=[row_block, row_block, pl.BlockSpec((1, *bounds.shape[1:]), lambda r, *_: (r, 0, 0))],
            out_specs=[pl.BlockSpec(shape, lambda r, *_: (r, 0, 0)) for shape in shapes],
        ),
        out_shape=[jax.ShapeDtypeStruct((rows, *shape[1:]), k.dtype) for shape in shapes],
        cost_estimate=pl.CostEstimate(flops=2000000, bytes_accessed=10 * k.size, transcendentals=0),
    )(table, k, v, bounds)


def attend_block(query, hot, low, steps, stride, keys, values, at):
    span, width = query.shape
    heads = width // HEAD_DIM
    owner = lax.broadcasted_iota(jnp.int32, (width, span), 0) // HEAD_DIM
    turned = query.T
    hot = hot.T
    sides = [
        jnp.concatenate([jnp.where(owner == head, turned, jnp.zeros_like(turned)), hot], axis=0)
        for head in range(heads)
    ]

    def step(index, held):
        start = pl.multiple_of(low + index * stride, LANES)
        key = keys[(*at, pl.ds(start, stride), slice(None))]
        result = []
        for head in range(heads):
            peak, total, summed = held[head]
            scores = jnp.dot(key, sides[head], preferred_element_type=jnp.float32)
            fresh = jnp.maximum(peak, jnp.max(scores, axis=0, keepdims=True))
            scale = jnp.exp(peak - fresh)
            expos = jnp.exp(scores - fresh)
            total = total * scale + jnp.sum(expos, axis=0, keepdims=True)
            value = values[(*at, slice(head * HEAD_DIM, (head + 1) * HEAD_DIM), pl.ds(start, stride))]
            summed = summed * scale + jnp.dot(value, expos.astype(jnp.bfloat16), preferred_element_type=jnp.float32)
            result.append((fresh, total, summed))
        return tuple(result)

    init = (
        jnp.full((1, span), 4 * MASKED, jnp.float32),
        jnp.zeros((1, span), jnp.float32),
        jnp.zeros((HEAD_DIM, span), jnp.float32),
    )
    done = lax.fori_loop(0, steps, step, (init,) * heads)
    whole = jnp.concatenate([summed / total for _, total, summed in done], axis=0)
    return whole.T.astype(jnp.bfloat16)


def attend_kernel(mode, table_ref, q_ref, keys_ref, values_ref, bounds_ref, *rest):
    if mode:
        more_ref, late_ref, before_ref, o_ref, keys, values, stage = rest
    else:
        o_ref = rest[0]
    half, _, count, width = q_ref.shape
    length = half * count
    span = max(SPAN, count)
    stride = min(STRIDE, length)
    slabs = span // count
    blocks = length // span
    row = pl.program_id(0)
    first = table_ref[row, 3 * blocks + 1] * length

    def entry(kind, block):
        return table_ref[row, kind * blocks + block]

    wanted = [entry(2, block) == mode for block in range(blocks)]
    if mode:
        begin, end = jnp.int32(2 * length), jnp.int32(0)
        for block in range(blocks):
            low = entry(0, block)
            begin = jnp.where(wanted[block], jnp.minimum(begin, low), begin)
            end = jnp.where(wanted[block], jnp.maximum(end, low + entry(1, block) * stride), end)

        def fetch(index, carry):
            at = pl.multiple_of(index * LANES, LANES)
            local = at - first
            mine = (local >= 0) & (local < length)

            @pl.when(mine)
            def _():
                inside = pl.ds(pl.multiple_of(local, LANES), LANES)
                keys[pl.ds(at, LANES), :] = keys_ref[0, inside, :]
                values[:, pl.ds(at, LANES)] = values_ref[0, :, inside]

            @pl.when(jnp.logical_not(mine))
            def _():
                room, extra = more_ref.shape[0], late_ref.shape[0]
                from_ = jnp.clip(table_ref[row, 3 * blocks] + at, 0, room + extra - LANES)
                for piece in range(0, LANES, PIECE):
                    one = from_ + piece

                    @pl.when(one < room)
                    def _():
                        stage[piece : piece + PIECE] = more_ref[pl.ds(pl.multiple_of(one, PIECE), PIECE), :]

                    @pl.when(one >= room)
                    def _():
                        stage[piece : piece + PIECE] = late_ref[pl.ds(pl.multiple_of(one - room, PIECE), PIECE), :]

                keys[pl.ds(at, LANES), :width] = stage[:, :width]
                keys[pl.ds(at, LANES), width:] = missing(bounds_ref, at, LANES)
                values[:, pl.ds(at, LANES)] = stage[:, width:].T

            return carry

        lax.fori_loop(begin // LANES, end // LANES, fetch, 0)

    for block in range(blocks):
        slab = pl.ds(block * slabs, slabs)

        @pl.when(wanted[block])
        def _():
            query = q_ref[slab, 0].reshape(span, width)
            hot = jnp.where(within(bounds_ref, 2, first + block * span, span), 1.0, 0.0).astype(jnp.bfloat16)
            low, steps = entry(0, block), entry(1, block)
            if mode:
                result = attend_block(query, hot, low, steps, stride, keys, values, ())
            else:
                low = jnp.minimum(low - first, length - steps * stride)
                result = attend_block(query, hot, low, steps, stride, keys_ref, values_ref, (0,))
            o_ref[slab, 0] = result.reshape(slabs, count, width)

        if mode:

            @pl.when(jnp.logical_not(wanted[block]))
            def _():
                o_ref[slab, 0] = before_ref[slab, 0]


def attend(mode, table, q, keys, values, bounds, *more):
    half, rows, count, width = q.shape
    length = half * count
    row_block = pl.BlockSpec((half, 1, count, width), lambda r, *_: (0, r, 0, 0))
    specs = [row_block]
    specs += [pl.BlockSpec((1, *x.shape[1:]), lambda r, *_: (r, 0, 0)) for x in (keys, values, bounds)]
    scratch = []
    if mode:
        specs += [pl.BlockSpec(x.shape, lambda r, *_: (0, 0)) for x in more[:2]] + [row_block]
        scratch = [
            pltpu.VMEM((2 * length, width + LANES), jnp.bfloat16),
            pltpu.VMEM((width, 2 * length), jnp.bfloat16),
            pltpu.VMEM((LANES, 2 * width), jnp.bfloat16),
        ]
    share = 4 if mode else 1
    return pl.pallas_call(
        functools.partial(attend_kernel, mode),
        grid_spec=pltpu.PrefetchScalarGridSpec(
            num_scalar_prefetch=1, grid=(rows,), in_specs=specs, out_specs=row_block, scratch_shapes=scratch
        ),
        out_shape=jax.ShapeDtypeStruct(q.shape, q.dtype),
        cost_estimate=pl.CostEstimate(
            flops=rows * width // HEAD_DIM * length * length * 128 // share,
            bytes_accessed=8 * rows * width * length,
            transcendentals=rows * length * length // 4 // share,
        ),
    )(table, q, keys, values, bounds, *more)


def tables(dec_rows, enc_rows, side):
    rows, whole = dec_rows.shape
    length = whole // 2
    blocks = length // SPAN
    stride = min(STRIDE, length)
    numbers = jnp.arange(LANES, dtype=jnp.int32)[None, :, None]
    bounds = []
    for ids in (enc_rows, dec_rows):
        bounds += [jnp.sum(ids[:, None, :] < numbers, axis=2), jnp.sum(ids[:, None, :] <= numbers, axis=2)]
    bounds = jnp.stack(bounds, axis=1).astype(jnp.int32)
    mine = lax.dynamic_slice(dec_rows, (0, side * length), (rows, length))
    docs = mine.reshape(rows, blocks, SPAN)
    starts = jnp.concatenate([docs[:, :, 0], dec_rows[:, length : length + 1]], axis=1)
    ends = jnp.concatenate([docs[:, :, -1], dec_rows[:, length - 1 : length]], axis=1)
    before = jnp.sum(enc_rows[:, None, :] < starts[:, :, None], axis=2, dtype=jnp.int32)
    upto = jnp.sum(enc_rows[:, None, :] <= ends[:, :, None], axis=2, dtype=jnp.int32)
    up = jnp.maximum(length - before[:, blocks], 0)
    down = jnp.maximum(upto[:, blocks] - length, 0)
    up, down = (-(-amount // PIECE) * PIECE for amount in (up, down))
    before, upto = before[:, :blocks], upto[:, :blocks]
    crosses = jnp.where(side == 0, upto > length, before < length).astype(jnp.int32)
    low = before // LANES * LANES
    steps = (upto - low + stride - 1) // stride
    low = jnp.minimum(low, whole - steps * stride)
    sent, got = jnp.where(side == 0, up, down), jnp.where(side == 0, down, up)
    offset_of = [PAD + jnp.cumsum(amount) - amount for amount in (sent, got)]
    first = jnp.where(side == 0, length - sent, 0)
    send = jnp.stack([offset_of[0], first, sent])
    base = offset_of[1] - jnp.where(side == 0, length, length - got)
    known = jnp.concatenate([low, steps, crosses, base[:, None], jnp.full((rows, 1), side, jnp.int32)], axis=1)
    return send, known, bounds, jnp.maximum(jnp.sum(up), jnp.sum(down))


def whole(queries, enc_keys, enc_values, dec_ids, enc_ids):
    group = lax.axis_size("seq")
    half = group // 2
    rows, count, _ = queries.shape
    length = half * count
    side = lax.axis_index("seq") // half
    k, v, dec_all, enc_all, q_packed = gather(queries, enc_keys, enc_values, dec_ids, enc_ids, group)
    sides = [list(range(half)), list(range(half, group))]

    def cross(block):
        return lax.ppermute(block, "seq", [(i, (i + half) % group) for i in range(group)])

    q = lax.all_to_all(q_packed, "seq", split_axis=0, concat_axis=0, axis_index_groups=sides, tiled=True)
    dec_rows, enc_rows = (x.transpose(1, 0, 2).reshape(rows, 2 * length) for x in (dec_all, enc_all))
    send, known, bounds, most = tables(dec_rows, enc_rows, side)
    trip = min(TRIP, length)
    full = rows * length + 2 * PAD
    room = full - (rows * length * (32 - ROOM) // 32 + trip - 1) // trip * trip
    main, rest = pack(send, k, v, room)
    more = cross(main)
    keys, values = prepare(known, k, v, bounds)
    most = lax.pmax(most, "dp")
    early = attend(0, known, q, keys, values, bounds)
    trips = (jnp.maximum(most + 2 * PAD - room, 0) + trip - 1) // trip
    more, early = lax.optimization_barrier((more, early))

    def one_trip(index, late):
        piece = cross(lax.dynamic_slice(rest, (index * trip, 0), (trip, rest.shape[1])))
        return lax.dynamic_update_slice(late, piece, (index * trip, 0))

    late = lax.fori_loop(0, trips, one_trip, jnp.zeros_like(rest))
    return give_back(attend(1, known, q, keys, values, bounds, more, late, early), group)


def solution(mesh):
    in_specs = (
        P("dp", "seq", None),
        P("dp", "seq", None),
        P("dp", "seq", None),
        P("dp", "seq"),
        P("dp", "seq"),
    )
    out_specs = P("dp", "seq", None)
    return jax.shard_map(whole, mesh=mesh, in_specs=in_specs, out_specs=out_specs, check_vma=False)
```

```python
import functools

import jax
import jax.numpy as jnp
from jax import lax
from jax.experimental import pallas as pl
from jax.experimental.pallas import tpu as pltpu
from jax.sharding import PartitionSpec as P


HEAD_DIM = 64
TALL = 80
DOCS = 16
LANES = 128
SPAN = 256
STRIDE = 512
PIECE = 32
TOGETHER = 4
MIB = 2**20
MASKED = -8192.0
ROOM = 11
TRIP = 512


def peer(me, shift, half):
    base = me // half * half
    return base + lax.rem(me - base + shift, half)


def greet(others):
    barrier = pltpu.get_barrier_semaphore()
    for target in others:
        pl.semaphore_signal(barrier, inc=1, device_id={"seq": target}, device_id_type=pl.DeviceIdType.MESH)
    pl.semaphore_wait(barrier, len(others))


def remote(src, dst, send_sem, recv_sem, target):
    return pltpu.make_async_remote_copy(
        src_ref=src,
        dst_ref=dst,
        send_sem=send_sem,
        recv_sem=recv_sem,
        device_id={"seq": target},
        device_id_type=pl.DeviceIdType.MESH,
    )


def gather_kernel(
    group, k_ref, v_ref, dec_ref, enc_ref, q_ref, k_out, v_out, dec_out, enc_out, q_out, held, ids_held, own_sem, ids_sem, send_sem, recv_sem, ids_send, ids_recv
):
    me = lax.axis_index("seq")
    half = group // 2
    width = k_out.shape[3]
    place = lax.rem(me, half)
    large = ((0, k_ref, k_out), (1, v_ref, v_out))
    small = ((0, dec_ref, dec_out), (1, enc_ref, enc_out))

    def columns(src, target):
        return src.at[:, :, pl.ds(pl.multiple_of(lax.rem(target, half) * width, LANES), width)]

    def heads(shift, slot, src, dst):
        target = peer(me, shift, half)
        at = slot * (half - 1) + shift - 1
        return remote(columns(src, target), dst.at[place], send_sem.at[at], recv_sem.at[at], target)

    def ids(shift, slot, src, dst):
        at = slot * (group - 1) + shift - 1
        return remote(src, dst.at[me], ids_send.at[at], ids_recv.at[at], lax.rem(me + shift, group))

    @pl.when(pl.program_id(0) == 0)
    def _():
        greet([lax.rem(me + shift, group) for shift in range(1, group)])
        for shift in range(1, group):
            for each in small:
                ids(shift, *each).start()
        for each in large:
            for shift in range(half - 1, 0, -1):
                heads(shift, *each).start()
        own = [pltpu.make_async_copy(columns(src, me), held.at[slot], own_sem.at[slot]) for slot, src, _ in large]
        own += [pltpu.make_async_copy(src, ids_held.at[slot], ids_sem.at[slot]) for slot, src, _ in small]
        for copy in own:
            copy.start()
        for copy in own:
            copy.wait()
        own = [pltpu.make_async_copy(held.at[slot], dst.at[place], own_sem.at[slot]) for slot, _, dst in large]
        own += [pltpu.make_async_copy(ids_held.at[slot], dst.at[me], ids_sem.at[slot]) for slot, _, dst in small]
        for copy in own:
            copy.start()
        for copy in own:
            copy.wait()

    for target in range(half):
        q_out[target, 0] = q_ref[0, :, target * width : (target + 1) * width]

    @pl.when(pl.program_id(0) == pl.num_programs(0) - 1)
    def _():
        for shift in range(1, group):
            for each in small:
                ids(shift, *each).wait()
        for each in large:
            for shift in range(1, half):
                heads(shift, *each).wait()


def gather(q, k, v, dec_ids, enc_ids, group):
    rows, count, features = k.shape
    half = group // 2
    width = features // half
    anywhere = pl.BlockSpec(memory_space=pltpu.HBM)
    block = pl.BlockSpec((1, count, features), lambda r: (r, 0, 0))
    packed = pl.BlockSpec((half, 1, count, width), lambda r: (0, r, 0, 0))
    spread = jax.ShapeDtypeStruct((half, rows, count, width), k.dtype)
    every = jax.ShapeDtypeStruct((group, rows, count), dec_ids.dtype)
    dma = pltpu.SemaphoreType.DMA
    return pl.pallas_call(
        functools.partial(gather_kernel, group),
        grid=(rows,),
        in_specs=[anywhere] * 4 + [block],
        out_specs=[anywhere] * 4 + [packed],
        out_shape=[spread, spread, every, every, spread],
        scratch_shapes=[
            pltpu.VMEM((2, rows, count, width), k.dtype),
            pltpu.VMEM((2, rows, count), dec_ids.dtype),
            dma((2,)),
            dma((2,)),
            dma((2 * (half - 1),)),
            dma((2 * (half - 1),)),
            dma((2 * (group - 1),)),
            dma((2 * (group - 1),)),
        ],
        compiler_params=pltpu.CompilerParams(collective_id=0, has_side_effects=True),
    )(k, v, dec_ids, enc_ids, q)


def give_back_kernel(group, o_ref, out_ref, held, own_sem, send_sem, recv_sem):
    me = lax.axis_index("seq")
    half = group // 2
    width = o_ref.shape[3]
    place = lax.rem(me, half)
    columns = out_ref.at[:, :, pl.ds(pl.multiple_of(place * width, LANES), width)]

    def transfer(shift):
        target = peer(me, shift, half)
        return remote(o_ref.at[lax.rem(target, half)], columns, send_sem.at[shift - 1], recv_sem.at[shift - 1], target)

    greet([peer(me, shift, half) for shift in range(1, half)])
    for shift in range(half - 1, 0, -1):
        transfer(shift).start()
    own = pltpu.make_async_copy(o_ref.at[place], held, own_sem)
    own.start()
    own.wait()
    own = pltpu.make_async_copy(held, columns, own_sem)
    own.start()
    own.wait()
    for shift in range(1, half):
        transfer(shift).wait()


def give_back(o, group):
    half, rows, count, width = o.shape
    return pl.pallas_call(
        functools.partial(give_back_kernel, group),
        in_specs=[pl.BlockSpec(memory_space=pltpu.HBM)],
        out_specs=pl.BlockSpec(memory_space=pltpu.HBM),
        out_shape=jax.ShapeDtypeStruct((rows, count, half * width), o.dtype),
        scratch_shapes=[
            pltpu.VMEM((rows, count, width), o.dtype),
            pltpu.SemaphoreType.DMA,
            pltpu.SemaphoreType.DMA((half - 1,)),
            pltpu.SemaphoreType.DMA((half - 1,)),
        ],
        compiler_params=pltpu.CompilerParams(collective_id=1, has_side_effects=True),
    )(o)


def pack_kernel(table_ref, shift_ref, k_ref, v_ref, o_ref):
    _, rows, count, width = k_ref.shape
    room = o_ref.shape[0]
    o_ref[...] = jnp.zeros(o_ref.shape, o_ref.dtype)

    def one_row(row, carry):
        offset, start, amount = table_ref[0, row] - shift_ref[0], table_ref[1, row], table_ref[2, row]

        def one(index):
            at = start + index * PIECE
            slab, inside = at // count, pl.ds(pl.multiple_of(at % count, PIECE), PIECE)
            into = pl.ds(pl.multiple_of(offset + index * PIECE, PIECE), PIECE)
            o_ref[into, :width] = k_ref[slab, row, inside, :]
            o_ref[into, width:] = v_ref[slab, row, inside, :]

        def move(index, carry):
            one(index)
            return carry

        def several(index, carry):
            for more in range(TOGETHER):
                one(lowest + index * TOGETHER + more)
            return carry

        lowest = jnp.maximum(-offset, 0) // PIECE
        highest = jnp.maximum(jnp.minimum(amount, room - offset) // PIECE, lowest)
        times = (highest - lowest) // TOGETHER
        lax.fori_loop(0, times, several, 0)
        return lax.fori_loop(lowest + times * TOGETHER, highest, move, carry)

    lax.fori_loop(0, rows, one_row, 0)


def pack(table, shift, k, v, room):
    width = k.shape[3]
    small, inside = pl.BlockSpec(memory_space=pltpu.SMEM), pl.BlockSpec(memory_space=pltpu.VMEM)
    return pl.pallas_call(
        pack_kernel,
        in_specs=[small] * 2 + [inside] * 2,
        out_specs=inside,
        out_shape=jax.ShapeDtypeStruct((room, 2 * width), k.dtype),
        cost_estimate=pl.CostEstimate(flops=2000000, bytes_accessed=8 * k.size, transcendentals=0),
    )(table, shift, k, v)


def within(low, high, at, amount):
    position = at + lax.broadcasted_iota(jnp.int32, (amount, LANES), 0)
    return (position >= low) & (position < high)


def missing(low, high, at, amount):
    documents = lax.broadcasted_iota(jnp.int32, (amount, LANES), 1)
    return jnp.where(within(low, high, at, amount) | (documents >= DOCS), 0.0, MASKED).astype(jnp.bfloat16)


def tall_values(turned):
    ones = jnp.ones((TALL - HEAD_DIM, turned.shape[1]), turned.dtype)
    return [jnp.concatenate([turned[at : at + HEAD_DIM], ones], axis=0) for at in range(0, turned.shape[0], HEAD_DIM)]


def prepare_kernel(table_ref, k_ref, v_ref, bounds_ref, keys, values, hot, _):
    half, _, count, width = k_ref.shape
    length = half * count
    first = table_ref[0, table_ref.shape[1] - 1] * length
    bounds = bounds_ref[0]
    keys[0, :, :width] = k_ref[:, 0].reshape(length, width)
    keys[0, :, width:] = missing(bounds[0:1], bounds[1:2], first, length)
    for head, part in enumerate(tall_values(v_ref[:, 0].reshape(length, width).T)):
        values[0, head * TALL : (head + 1) * TALL] = part
    here = jnp.where(within(bounds[2:3], bounds[3:4], first, length), 1.0, 0.0).astype(jnp.bfloat16).T
    hot[0] = here[:DOCS]


def prepare(table, k, v, bounds, extra):
    half, rows, count, width = k.shape
    length = half * count
    row_block = pl.BlockSpec((half, 1, count, width), lambda r, *_: (0, r, 0, 0))
    shapes = [(length, width + LANES), (width // HEAD_DIM * TALL, length), (DOCS, length)]
    return pl.pallas_call(
        prepare_kernel,
        grid_spec=pltpu.PrefetchScalarGridSpec(
            num_scalar_prefetch=1,
            grid=(rows,),
            in_specs=[row_block, row_block, pl.BlockSpec((1, *bounds.shape[1:]), lambda r, *_: (r, 0, 0))],
            out_specs=[pl.BlockSpec((1, *shape), lambda r, *_: (r, 0, 0)) for shape in shapes]
            + [pl.BlockSpec(memory_space=pltpu.HBM)],
        ),
        out_shape=[jax.ShapeDtypeStruct((rows, *shape), k.dtype) for shape in shapes]
        + [jax.ShapeDtypeStruct((extra, 2 * width), k.dtype)],
        cost_estimate=pl.CostEstimate(flops=2000000, bytes_accessed=10 * k.size, transcendentals=0),
    )(table, k, v, bounds)


def attend_kernel(mode, table_ref, *refs):
    if mode:
        trips_ref, bounds_ref, q_from, hot_from, peak_from, sum_from, more_from, late_from, _, o_to, *scratch = refs
        items, even, odd, even_peak, odd_peak, peak_of, sum_of, peak_now, sum_now, q_ref, hot_ref, o_ref, more_ref, sem = scratch
    else:
        q_ref, keys, values, hot_ref, o_ref, peak_of, sum_of, items, even, odd, even_peak, odd_peak = refs
    half, rows, count, width = q_ref.shape
    length = half * count
    heads = width // HEAD_DIM
    _, stride, span = even.shape
    slabs = span // count
    blocks = length // span
    side = table_ref[0, 4 * blocks + 1]

    def entry(row, kind, block):
        return table_ref[row, kind * blocks + block]

    def each_block(do):
        def one(number, carry):
            row, block = number // blocks, number % blocks

            @pl.when(entry(row, 3, block) > 0)
            def _():
                do(number, row, pl.ds(block * slabs, slabs))

            return carry

        lax.fori_loop(0, rows * blocks, one, 0)

    if mode:
        room = more_from.shape[0]
        avail = room + trips_ref[0] * trips_ref[1]

        def move(finish):
            def block(number, row, slab):
                for src, dst in (
                    (q_from.at[slab, row], q_ref.at[slab, row]),
                    (peak_from.at[number], peak_of.at[number]),
                    (sum_from.at[number], sum_of.at[number]),
                ):
                    copy = pltpu.make_async_copy(src, dst, sem)
                    copy.wait() if finish else copy.start()

            for src, dst in ((more_from, more_ref.at[pl.ds(0, room)]), (hot_from, hot_ref)):
                copy = pltpu.make_async_copy(src, dst, sem)
                copy.wait() if finish else copy.start()
            each_block(block)

        move(False)

    def list_block(number, total):
        row, block = number // blocks, number % blocks
        steps = entry(row, 2 * mode + 1, block)
        low = entry(row, 2 * mode, block)
        if mode:
            low = jnp.minimum(low, avail - steps * stride)
        else:

            @pl.when(steps == 0)
            def _():
                peak_of[number] = jnp.full(peak_of.shape[1:], 4 * MASKED, jnp.float32)
                sum_of[number] = jnp.zeros(sum_of.shape[1:], jnp.float32)

        def list_step(index, total):
            items[0, total] = row
            items[1, total] = block
            items[2, total] = low + index * stride
            items[3, total] = (index == 0).astype(jnp.int32)
            return total + 1

        return lax.fori_loop(0, steps, list_step, total)

    total = lax.fori_loop(0, rows * blocks, list_block, jnp.int32(1))
    if mode:

        @pl.when(trips_ref[0] > 0)
        def _():
            pltpu.sync_copy(late_from, more_ref.at[pl.ds(room, late_from.shape[0])])

        move(True)

    def score(index, scores, peaks):
        row, block = items[0, index], items[1, index]
        query = q_ref[pl.ds(block * slabs, slabs), row].reshape(span, width).T
        here = hot_ref[row, :, pl.ds(pl.multiple_of(block * span, span), span)]
        owner = lax.broadcasted_iota(jnp.int32, (width, span), 0) // HEAD_DIM
        nothing = jnp.zeros((LANES - DOCS, span), jnp.bfloat16)
        if mode:
            start = pl.multiple_of(items[2, index], PIECE)
            low, high = bounds_ref[row, 0:1], bounds_ref[row, 1:2]
            low = jnp.where(side == 0, jnp.maximum(low, length), low)
            high = jnp.where(side == 0, high, jnp.minimum(high, length))
            miss = missing(low, high, start - table_ref[row, 4 * blocks], stride)
            key = jnp.concatenate([more_ref[pl.ds(start, stride), :width], miss], axis=1)
        else:
            start = pl.multiple_of(items[2, index], LANES)
            key = keys[row, pl.ds(start, stride), :]
        for head in range(heads):
            one = jnp.where(owner == head, query, jnp.zeros_like(query))
            result = jnp.dot(key, jnp.concatenate([one, here, nothing], axis=0), preferred_element_type=jnp.float32)
            scores[head] = result
            peaks[head] = jnp.max(result, axis=0, keepdims=True)

    def weigh(index, scores, peaks):
        row, block = items[0, index], items[1, index]
        number, fresh_start = row * blocks + block, items[3, index] == 1
        if mode:
            start = pl.multiple_of(items[2, index], PIECE)
            value = tall_values(more_ref[pl.ds(start, stride), width:].T)
        else:
            start = pl.multiple_of(items[2, index], LANES)
            value = [values[row, head * TALL : (head + 1) * TALL, pl.ds(start, stride)] for head in range(heads)]
        now, at = ((peak_now, sum_now), 0) if mode else ((peak_of, sum_of), number)
        done = []
        for head in range(heads):
            peak, before = (x[at, head] for x in now)
            began = (peak_of[number, head], sum_of[number, head]) if mode else (4 * MASKED, 0.0)
            peak, before = jnp.where(fresh_start, began[0], peak), jnp.where(fresh_start, began[1], before)
            fresh = jnp.maximum(peak, peaks[head])
            now[0][at, head] = fresh
            expos = jnp.exp(scores[head] - fresh).astype(jnp.bfloat16)
            summed = before * jnp.exp(peak - fresh) + jnp.dot(value[head], expos, preferred_element_type=jnp.float32)
            now[1][at, head] = summed
            done.append(summed[:HEAD_DIM] / summed[HEAD_DIM : HEAD_DIM + 1])
        whole = jnp.concatenate(done, axis=0).T.astype(jnp.bfloat16)
        o_ref[pl.ds(block * slabs, slabs), row] = whole.reshape(slabs, count, width)

    @pl.when(total > 1)
    def _():
        begin = total % 2
        for field in range(4):
            items[field, 0] = items[field, 1]
        score(begin, even, even_peak)

        def pair(index, carry):
            at = begin + 2 * index
            score(at + 1, odd, odd_peak)
            weigh(at, even, even_peak)
            score(jnp.minimum(at + 2, total - 1), even, even_peak)
            weigh(at + 1, odd, odd_peak)
            return carry

        lax.fori_loop(0, (total - begin) // 2, pair, 0)

    if mode:

        def put(finish):
            def block(number, row, slab):
                copy = pltpu.make_async_copy(o_ref.at[slab, row], o_to.at[slab, row], sem)
                copy.wait() if finish else copy.start()

            each_block(block)

        put(False)
        put(True)


def attend(mode, table, q, *more):
    half, rows, count, width = q.shape
    length = half * count
    heads = width // HEAD_DIM
    span = max(SPAN, count)
    stride = min(STRIDE, length)
    small = pl.BlockSpec(memory_space=pltpu.SMEM)
    inside = pl.BlockSpec(memory_space=pltpu.VMEM)
    outside = pl.BlockSpec(memory_space=pltpu.HBM)
    numbers = rows * (length // span)
    state = [(numbers, heads, 1, span), (numbers, heads, TALL, span)]
    scratch = [
        pltpu.SMEM((4, numbers * (2 * length // stride + 1) + 1), jnp.int32),
        pltpu.VMEM((heads, stride, span), jnp.float32),
        pltpu.VMEM((heads, stride, span), jnp.float32),
        pltpu.VMEM((heads, 1, span), jnp.float32),
        pltpu.VMEM((heads, 1, span), jnp.float32),
    ]
    shapes = [jax.ShapeDtypeStruct(q.shape, q.dtype)]
    if mode:
        trips, bounds, hot, peak, summed, cross, late, early = more
        scratch += [pltpu.VMEM(shape, jnp.float32) for shape in state + [(1, *shape[1:]) for shape in state]]
        scratch += [
            pltpu.VMEM(q.shape, q.dtype),
            pltpu.VMEM(hot.shape, q.dtype),
            pltpu.VMEM(q.shape, q.dtype),
            pltpu.VMEM((cross.shape[0] + late.shape[0], 2 * width), q.dtype),
            pltpu.SemaphoreType.DMA,
        ]
        args = (table, trips, bounds, q, hot, peak, summed, cross, late, early)
        specs, out_specs = [small] * 2 + [inside] + [outside] * 7, [outside]
    else:
        keys, values, hot = more
        args = (table, q, keys, values, hot)
        specs, out_specs = [small] + [inside] * 4, [inside] * 3
        shapes += [jax.ShapeDtypeStruct(shape, jnp.float32) for shape in state]
    share = 4 if mode else 1
    return pl.pallas_call(
        functools.partial(attend_kernel, mode),
        in_specs=specs,
        out_specs=out_specs,
        out_shape=shapes,
        input_output_aliases={9: 0} if mode else {},
        scratch_shapes=scratch,
        compiler_params=pltpu.CompilerParams(vmem_limit_bytes=60 * MIB),
        cost_estimate=pl.CostEstimate(
            flops=rows * heads * length * length * 128 // share,
            bytes_accessed=8 * rows * width * length,
            transcendentals=rows * length * length // 4 // share,
        ),
    )(*args)


def tables(dec_rows, enc_rows, side):
    rows, whole = dec_rows.shape
    length = whole // 2
    blocks = length // SPAN
    stride = min(STRIDE, length)
    numbers = jnp.arange(LANES, dtype=jnp.int32)[None, :, None]
    bounds = []
    for ids in (enc_rows, dec_rows):
        bounds += [jnp.sum(ids[:, None, :] < numbers, axis=2), jnp.sum(ids[:, None, :] <= numbers, axis=2)]
    bounds = jnp.stack(bounds, axis=1).astype(jnp.int32)
    mine = lax.dynamic_slice(dec_rows, (0, side * length), (rows, length))
    docs = mine.reshape(rows, blocks, SPAN)
    starts = jnp.concatenate([docs[:, :, 0], dec_rows[:, length : length + 1]], axis=1)
    ends = jnp.concatenate([docs[:, :, -1], dec_rows[:, length - 1 : length]], axis=1)
    before = jnp.sum(enc_rows[:, None, :] < starts[:, :, None], axis=2, dtype=jnp.int32)
    upto = jnp.sum(enc_rows[:, None, :] <= ends[:, :, None], axis=2, dtype=jnp.int32)
    up = jnp.maximum(length - before[:, blocks], 0)
    down = jnp.maximum(upto[:, blocks] - length, 0)
    up, down = (-(-amount // PIECE) * PIECE for amount in (up, down))
    before, upto = before[:, :blocks], upto[:, :blocks]
    sent, got = jnp.where(side == 0, up, down), jnp.where(side == 0, down, up)
    offset_of = [jnp.cumsum(amount) - amount for amount in (sent, got)]
    first = jnp.where(side == 0, length - sent, 0)
    send = jnp.stack([offset_of[0], first, sent])
    base = (offset_of[1] - jnp.where(side == 0, length, length - got))[:, None]
    home = side * length
    near, far = jnp.maximum(before - home, 0), jnp.minimum(upto - home, length)
    low = near // LANES * LANES
    steps = jnp.where(far > near, (far - low + stride - 1) // stride, 0)
    low = jnp.minimum(low, length - steps * stride)
    near = base + jnp.where(side == 0, jnp.maximum(before, length), before)
    far = base + jnp.where(side == 0, upto, jnp.minimum(upto, length))
    start = near // PIECE * PIECE
    more = jnp.where(far > near, (far - start + stride - 1) // stride, 0)
    known = jnp.concatenate([low, steps, start, more, base, jnp.full((rows, 1), side, jnp.int32)], axis=1)
    return send, known, bounds, jnp.maximum(jnp.sum(up), jnp.sum(down))


def whole(queries, enc_keys, enc_values, dec_ids, enc_ids):
    group = lax.axis_size("seq")
    half = group // 2
    rows, count, _ = queries.shape
    length = half * count
    side = lax.axis_index("seq") // half
    k, v, dec_all, enc_all, q_packed = gather(queries, enc_keys, enc_values, dec_ids, enc_ids, group)
    sides = [list(range(half)), list(range(half, group))]

    def cross(block):
        return lax.ppermute(block, "seq", [(i, (i + half) % group) for i in range(group)])

    q = lax.all_to_all(q_packed, "seq", split_axis=0, concat_axis=0, axis_index_groups=sides, tiled=True)
    dec_rows, enc_rows = (x.transpose(1, 0, 2).reshape(rows, 2 * length) for x in (dec_all, enc_all))
    send, known, bounds, most = tables(dec_rows, enc_rows, side)
    trip = min(TRIP, length)
    full = rows * length
    room = full * ROOM // 32 // LANES * LANES
    extra = -(-(full - room) // trip) * trip
    more = cross(pack(send, jnp.zeros((1,), jnp.int32), k, v, room))
    q = lax.all_to_all(q_packed, "seq", split_axis=0, concat_axis=0, axis_index_groups=sides, tiled=True)
    keys, values, hot, empty = prepare(known, k, v, bounds, extra)
    most = lax.pmax(most, "dp")
    early, peak, summed = attend(0, known, q, keys, values, hot)
    trips = (jnp.maximum(most - room, 0) + trip - 1) // trip
    more, early = lax.optimization_barrier((more, early))

    def one_trip(index, late):
        piece = cross(pack(send, jnp.full((1,), room + index * trip, jnp.int32), k, v, trip))
        return lax.dynamic_update_slice(late, piece, (index * trip, 0))

    late = lax.fori_loop(0, trips, one_trip, empty)
    sent_late = jnp.stack([trips, jnp.full_like(trips, trip)])
    out = attend(1, known, q, sent_late, bounds, hot, peak, summed, more, late, early)[0]
    return give_back(out, group)


def solution(mesh):
    in_specs = (
        P("dp", "seq", None),
        P("dp", "seq", None),
        P("dp", "seq", None),
        P("dp", "seq"),
        P("dp", "seq"),
    )
    out_specs = P("dp", "seq", None)
    return jax.shard_map(whole, mesh=mesh, in_specs=in_specs, out_specs=out_specs, check_vma=False)
```

```python
import functools

import jax
import jax.numpy as jnp
from jax import lax
from jax.experimental import pallas as pl
from jax.experimental.pallas import tpu as pltpu
from jax.sharding import PartitionSpec as P


HEAD_DIM = 64
TALL = 80
DOCS = 16
LANES = 128
SPAN = 256
STRIDE = (512, 256)
PIECE = 16
TOGETHER = 8
MIB = 2**20
MASKED = -8192.0
ROOM = 11
TRIP = 512


def peer(me, shift, half):
    base, place = me // half * half, lax.rem(me, half)
    if half & (half - 1):
        return base + lax.rem(place + shift, half)
    bit, flipped = 1, 0
    while bit < half:
        flipped += bit * lax.rem(place // bit + shift // bit, 2)
        bit *= 2
    return base + flipped


def greet(others):
    barrier = pltpu.get_barrier_semaphore()
    for target in others:
        pl.semaphore_signal(barrier, inc=1, device_id={"seq": target}, device_id_type=pl.DeviceIdType.MESH)
    pl.semaphore_wait(barrier, len(others))


def remote(src, dst, send_sem, recv_sem, target):
    return pltpu.make_async_remote_copy(
        src_ref=src,
        dst_ref=dst,
        send_sem=send_sem,
        recv_sem=recv_sem,
        device_id={"seq": target},
        device_id_type=pl.DeviceIdType.MESH,
    )


def gather_kernel(
    group, k_ref, v_ref, dec_ref, enc_ref, q_ref, k_out, v_out, ids_out, q_out, held, ids_held, own_sem, ids_sem, send_sem, recv_sem, ids_send, ids_recv
):
    me = lax.axis_index("seq")
    half = group // 2
    width = k_out.shape[3]
    place = lax.rem(me, half)
    large = ((0, k_ref, k_out), (1, v_ref, v_out))

    def columns(src, target):
        return src.at[:, :, pl.ds(pl.multiple_of(lax.rem(target, half) * width, LANES), width)]

    def heads(shift, slot, src, dst):
        target = peer(me, shift, half)
        at = slot * (half - 1) + shift - 1
        return remote(columns(src, target), dst.at[place], send_sem.at[at], recv_sem.at[at], target)

    def ids(shift):
        at = shift - 1
        return remote(ids_held, ids_out.at[me], ids_send.at[at], ids_recv.at[at], lax.rem(me + shift, group))

    @pl.when(pl.program_id(0) == 0)
    def _():
        own_ids = [
            pltpu.make_async_copy(src, ids_held.at[slot], ids_sem.at[slot]) for slot, src in enumerate((dec_ref, enc_ref))
        ]
        for copy in own_ids:
            copy.start()
        greet([lax.rem(me + shift, group) for shift in range(1, group)])
        for copy in own_ids:
            copy.wait()
        for shift in range(1, half):
            for each in large:
                heads(shift, *each).start()
        for shift in range(1, group):
            ids(shift).start()
        own = [pltpu.make_async_copy(columns(src, me), held.at[slot], own_sem.at[slot]) for slot, src, _ in large]
        own += [pltpu.make_async_copy(ids_held, ids_out.at[me], ids_sem.at[0])]
        for copy in own:
            copy.start()
        for copy in own:
            copy.wait()
        own = [pltpu.make_async_copy(held.at[slot], dst.at[place], own_sem.at[slot]) for slot, _, dst in large]
        for copy in own:
            copy.start()
        for copy in own:
            copy.wait()

    for target in range(half):
        q_out[target, 0] = q_ref[0, :, target * width : (target + 1) * width]

    @pl.when(pl.program_id(0) == pl.num_programs(0) - 1)
    def _():
        for shift in range(1, group):
            ids(shift).wait()
        for each in large:
            for shift in range(1, half):
                heads(shift, *each).wait()


def gather(q, k, v, dec_ids, enc_ids, group):
    rows, count, features = k.shape
    half = group // 2
    width = features // half
    anywhere = pl.BlockSpec(memory_space=pltpu.HBM)
    block = pl.BlockSpec((1, count, features), lambda r: (r, 0, 0))
    packed = pl.BlockSpec((half, 1, count, width), lambda r: (0, r, 0, 0))
    spread = jax.ShapeDtypeStruct((half, rows, count, width), k.dtype)
    every = jax.ShapeDtypeStruct((group, 2, rows, count), dec_ids.dtype)
    dma = pltpu.SemaphoreType.DMA
    return pl.pallas_call(
        functools.partial(gather_kernel, group),
        grid=(rows,),
        in_specs=[anywhere] * 4 + [block],
        out_specs=[anywhere] * 3 + [packed],
        out_shape=[spread, spread, every, spread],
        scratch_shapes=[
            pltpu.VMEM((2, rows, count, width), k.dtype),
            pltpu.VMEM((2, rows, count), dec_ids.dtype),
            dma((2,)),
            dma((2,)),
            dma((2 * (half - 1),)),
            dma((2 * (half - 1),)),
            dma((group - 1,)),
            dma((group - 1,)),
        ],
        compiler_params=pltpu.CompilerParams(collective_id=0, has_side_effects=True),
    )(k, v, dec_ids, enc_ids, q)


def give_back_kernel(group, o_ref, out_ref, held, own_sem, send_sem, recv_sem):
    me = lax.axis_index("seq")
    half = group // 2
    width = o_ref.shape[3]
    place = lax.rem(me, half)
    columns = out_ref.at[:, :, pl.ds(pl.multiple_of(place * width, LANES), width)]

    def transfer(shift):
        target = peer(me, shift, half)
        return remote(o_ref.at[lax.rem(target, half)], columns, send_sem.at[shift - 1], recv_sem.at[shift - 1], target)

    greet([peer(me, shift, half) for shift in range(1, half)])
    for shift in range(1, half):
        transfer(shift).start()
    own = pltpu.make_async_copy(o_ref.at[place], held, own_sem)
    own.start()
    own.wait()
    own = pltpu.make_async_copy(held, columns, own_sem)
    own.start()
    own.wait()
    for shift in range(1, half):
        transfer(shift).wait()


def give_back(o, group):
    half, rows, count, width = o.shape
    return pl.pallas_call(
        functools.partial(give_back_kernel, group),
        in_specs=[pl.BlockSpec(memory_space=pltpu.HBM)],
        out_specs=pl.BlockSpec(memory_space=pltpu.HBM),
        out_shape=jax.ShapeDtypeStruct((rows, count, half * width), o.dtype),
        scratch_shapes=[
            pltpu.VMEM((rows, count, width), o.dtype),
            pltpu.SemaphoreType.DMA,
            pltpu.SemaphoreType.DMA((half - 1,)),
            pltpu.SemaphoreType.DMA((half - 1,)),
        ],
        compiler_params=pltpu.CompilerParams(collective_id=1, has_side_effects=True),
    )(o)


def pack_kernel(table_ref, shift_ref, k_ref, v_ref, o_ref):
    _, rows, count, width = k_ref.shape
    room = o_ref.shape[0]
    o_ref[...] = jnp.zeros(o_ref.shape, o_ref.dtype)

    def one_row(row, carry):
        offset, start, amount = table_ref[0, row] - shift_ref[0], table_ref[1, row], table_ref[2, row]

        def one(index):
            at = start + index * PIECE
            slab, inside = at // count, pl.ds(pl.multiple_of(at % count, PIECE), PIECE)
            into = pl.ds(pl.multiple_of(offset + index * PIECE, PIECE), PIECE)
            o_ref[into, :width] = k_ref[slab, row, inside, :]
            o_ref[into, width:] = v_ref[slab, row, inside, :]

        def move(index, carry):
            one(index)
            return carry

        def several(index, carry):
            for more in range(TOGETHER):
                one(lowest + index * TOGETHER + more)
            return carry

        lowest = jnp.maximum(-offset, 0) // PIECE
        highest = jnp.maximum(jnp.minimum(amount, room - offset) // PIECE, lowest)
        times = (highest - lowest) // TOGETHER
        lax.fori_loop(0, times, several, 0)
        return lax.fori_loop(lowest + times * TOGETHER, highest, move, carry)

    lax.fori_loop(0, rows, one_row, 0)


def pack(table, shift, k, v, room):
    width = k.shape[3]
    small, inside = pl.BlockSpec(memory_space=pltpu.SMEM), pl.BlockSpec(memory_space=pltpu.VMEM)
    return pl.pallas_call(
        pack_kernel,
        in_specs=[small] * 2 + [inside] * 2,
        out_specs=inside,
        out_shape=jax.ShapeDtypeStruct((room, 2 * width), k.dtype),
        compiler_params=pltpu.CompilerParams(vmem_limit_bytes=16 * MIB),
        cost_estimate=pl.CostEstimate(flops=2000000, bytes_accessed=8 * k.size, transcendentals=0),
    )(table, shift, k, v)


def within(low, high, at, amount):
    position = at + lax.broadcasted_iota(jnp.int32, (amount, LANES), 0)
    return (position >= low) & (position < high)


def missing(low, high, at, amount):
    documents = lax.broadcasted_iota(jnp.int32, (amount, LANES), 1)
    return jnp.where(within(low, high, at, amount) | (documents >= DOCS), 0.0, MASKED).astype(jnp.bfloat16)


def tall_values(turned):
    ones = jnp.ones((TALL - HEAD_DIM, turned.shape[1]), turned.dtype)
    return [jnp.concatenate([turned[at : at + HEAD_DIM], ones], axis=0) for at in range(0, turned.shape[0], HEAD_DIM)]


def prepare_kernel(table_ref, k_ref, v_ref, bounds_ref, keys, values, hot, _):
    half, _, count, width = k_ref.shape
    length = half * count
    first = table_ref[table_ref.shape[0] - 1, 0] * length
    bounds = bounds_ref[0]
    keys[0, :, :width] = k_ref[:, 0].reshape(length, width)
    keys[0, :, width:] = missing(bounds[0:1], bounds[1:2], first, length)
    for head, part in enumerate(tall_values(v_ref[:, 0].reshape(length, width).T)):
        values[0, head * TALL : (head + 1) * TALL] = part
    here = jnp.where(within(bounds[2:3], bounds[3:4], first, length), 1.0, 0.0).astype(jnp.bfloat16).T
    hot[0] = here[:DOCS]


def prepare(table, k, v, bounds, extra):
    half, rows, count, width = k.shape
    length = half * count
    row_block = pl.BlockSpec((half, 1, count, width), lambda r, *_: (0, r, 0, 0))
    shapes = [(length, width + LANES), (width // HEAD_DIM * TALL, length), (DOCS, length)]
    return pl.pallas_call(
        prepare_kernel,
        grid_spec=pltpu.PrefetchScalarGridSpec(
            num_scalar_prefetch=1,
            grid=(rows,),
            in_specs=[row_block, row_block, pl.BlockSpec((1, *bounds.shape[1:]), lambda r, *_: (r, 0, 0))],
            out_specs=[pl.BlockSpec((1, *shape), lambda r, *_: (r, 0, 0)) for shape in shapes]
            + [pl.BlockSpec(memory_space=pltpu.HBM)],
        ),
        out_shape=[jax.ShapeDtypeStruct((rows, *shape), k.dtype) for shape in shapes]
        + [jax.ShapeDtypeStruct((extra, 2 * width), k.dtype)],
        cost_estimate=pl.CostEstimate(flops=2000000, bytes_accessed=10 * k.size, transcendentals=0),
    )(table, k, v, bounds)


def attend_kernel(mode, table_ref, *refs):
    if mode:
        trips_ref, bounds_ref, q_from, hot_from, peak_from, sum_from, more_from, late_from, _, o_to, *scratch = refs
        items, even, odd, even_peak, odd_peak, peak_of, sum_of, peak_now, sum_now, q_ref, hot_ref, o_ref, more_ref, sem = scratch
    else:
        q_ref, keys, values, hot_ref, o_ref, peak_of, sum_of, items, even, odd, even_peak, odd_peak = refs
    half, rows, count, width = q_ref.shape
    length = half * count
    heads = width // HEAD_DIM
    _, stride, span = even.shape
    slabs = span // count
    blocks = length // span
    side = table_ref[4 * blocks + 1, 0]

    def entry(row, kind, block):
        return table_ref[kind * blocks + block, row]

    def each_block(do):
        def one(number, carry):
            row, block = number // blocks, number % blocks

            @pl.when(entry(row, 3, block) > 0)
            def _():
                do(number, row, pl.ds(block * slabs, slabs))

            return carry

        lax.fori_loop(0, rows * blocks, one, 0)

    if mode:
        room = more_from.shape[0]
        avail = room + trips_ref[0] * trips_ref[1]

        def move(finish):
            def block(number, row, slab):
                for src, dst in (
                    (q_from.at[slab, row], q_ref.at[slab, row]),
                    (peak_from.at[number], peak_of.at[number]),
                    (sum_from.at[number], sum_of.at[number]),
                ):
                    copy = pltpu.make_async_copy(src, dst, sem)
                    copy.wait() if finish else copy.start()

            for src, dst in ((more_from, more_ref.at[pl.ds(0, room)]), (hot_from, hot_ref)):
                copy = pltpu.make_async_copy(src, dst, sem)
                copy.wait() if finish else copy.start()
            each_block(block)

        move(False)

    def list_block(number, total):
        row, block = number // blocks, number % blocks
        steps = entry(row, 2 * mode + 1, block)
        low = entry(row, 2 * mode, block)
        if mode:
            low = jnp.minimum(low, avail - steps * stride)
        else:

            @pl.when(steps == 0)
            def _():
                peak_of[number] = jnp.full(peak_of.shape[1:], 4 * MASKED, jnp.float32)
                sum_of[number] = jnp.zeros(sum_of.shape[1:], jnp.float32)

        def list_step(index, total):
            items[0, total] = row
            items[1, total] = block
            items[2, total] = low + index * stride
            items[3, total] = (index == 0).astype(jnp.int32)
            return total + 1

        return lax.fori_loop(0, steps, list_step, total)

    total = lax.fori_loop(0, rows * blocks, list_block, jnp.int32(1))
    if mode:

        @pl.when(trips_ref[0] > 0)
        def _():
            pltpu.sync_copy(late_from, more_ref.at[pl.ds(room, late_from.shape[0])])

        move(True)

    def score(index, scores, peaks):
        row, block = items[0, index], items[1, index]
        query = q_ref[pl.ds(block * slabs, slabs), row].reshape(span, width).T
        here = hot_ref[row, :, pl.ds(pl.multiple_of(block * span, span), span)]
        owner = lax.broadcasted_iota(jnp.int32, (width, span), 0) // HEAD_DIM
        nothing = jnp.zeros((LANES - DOCS, span), jnp.bfloat16)
        if mode:
            start = pl.multiple_of(items[2, index], PIECE)
            low, high = bounds_ref[row, 0:1], bounds_ref[row, 1:2]
            low = jnp.where(side == 0, jnp.maximum(low, length), low)
            high = jnp.where(side == 0, high, jnp.minimum(high, length))
            miss = missing(low, high, start - table_ref[4 * blocks, row], stride)
            key = jnp.concatenate([more_ref[pl.ds(start, stride), :width], miss], axis=1)
        else:
            start = pl.multiple_of(items[2, index], LANES)
            key = keys[row, pl.ds(start, stride), :]
        for head in range(heads):
            one = jnp.where(owner == head, query, jnp.zeros_like(query))
            result = jnp.dot(key, jnp.concatenate([one, here, nothing], axis=0), preferred_element_type=jnp.float32)
            scores[head] = result
            peaks[head] = jnp.max(result, axis=0, keepdims=True)

    def weigh(index, scores, peaks):
        row, block = items[0, index], items[1, index]
        number, fresh_start = row * blocks + block, items[3, index] == 1
        if mode:
            start = pl.multiple_of(items[2, index], PIECE)
            value = tall_values(more_ref[pl.ds(start, stride), width:].T)
        else:
            start = pl.multiple_of(items[2, index], LANES)
            value = [values[row, head * TALL : (head + 1) * TALL, pl.ds(start, stride)] for head in range(heads)]
        now, at = ((peak_now, sum_now), 0) if mode else ((peak_of, sum_of), number)
        done = []
        for head in range(heads):
            peak, before = (x[at, head] for x in now)
            began = (peak_of[number, head], sum_of[number, head]) if mode else (4 * MASKED, 0.0)
            peak, before = jnp.where(fresh_start, began[0], peak), jnp.where(fresh_start, began[1], before)
            fresh = jnp.maximum(peak, peaks[head])
            now[0][at, head] = fresh
            expos = jnp.exp(scores[head] - fresh).astype(jnp.bfloat16)
            summed = before * jnp.exp(peak - fresh) + jnp.dot(value[head], expos, preferred_element_type=jnp.float32)
            now[1][at, head] = summed
            done.append(summed[:HEAD_DIM] / summed[HEAD_DIM : HEAD_DIM + 1])
        whole = jnp.concatenate(done, axis=0).T.astype(jnp.bfloat16)
        o_ref[pl.ds(block * slabs, slabs), row] = whole.reshape(slabs, count, width)

    @pl.when(total > 1)
    def _():
        begin = total % 2
        for field in range(4):
            items[field, 0] = items[field, 1]
        score(begin, even, even_peak)

        def pair(index, carry):
            at = begin + 2 * index
            score(at + 1, odd, odd_peak)
            weigh(at, even, even_peak)
            score(jnp.minimum(at + 2, total - 1), even, even_peak)
            weigh(at + 1, odd, odd_peak)
            return carry

        lax.fori_loop(0, (total - begin) // 2, pair, 0)

    if mode:

        def put(finish):
            def block(number, row, slab):
                copy = pltpu.make_async_copy(o_ref.at[slab, row], o_to.at[slab, row], sem)
                copy.wait() if finish else copy.start()

            each_block(block)

        put(False)
        put(True)


def attend(mode, table, q, *more):
    half, rows, count, width = q.shape
    length = half * count
    heads = width // HEAD_DIM
    span = max(SPAN, count)
    stride = min(STRIDE[mode], length)
    small = pl.BlockSpec(memory_space=pltpu.SMEM)
    inside = pl.BlockSpec(memory_space=pltpu.VMEM)
    outside = pl.BlockSpec(memory_space=pltpu.HBM)
    numbers = rows * (length // span)
    state = [(numbers, heads, 1, span), (numbers, heads, TALL, span)]
    scratch = [
        pltpu.SMEM((4, numbers * (2 * length // stride + 1) + 1), jnp.int32),
        pltpu.VMEM((heads, stride, span), jnp.float32),
        pltpu.VMEM((heads, stride, span), jnp.float32),
        pltpu.VMEM((heads, 1, span), jnp.float32),
        pltpu.VMEM((heads, 1, span), jnp.float32),
    ]
    shapes = [jax.ShapeDtypeStruct(q.shape, q.dtype)]
    if mode:
        trips, bounds, hot, peak, summed, cross, late, early = more
        scratch += [pltpu.VMEM(shape, jnp.float32) for shape in state + [(1, *shape[1:]) for shape in state]]
        scratch += [
            pltpu.VMEM(q.shape, q.dtype),
            pltpu.VMEM(hot.shape, q.dtype),
            pltpu.VMEM(q.shape, q.dtype),
            pltpu.VMEM((cross.shape[0] + late.shape[0], 2 * width), q.dtype),
            pltpu.SemaphoreType.DMA,
        ]
        args = (table, trips, bounds, q, hot, peak, summed, cross, late, early)
        specs, out_specs = [small] * 2 + [inside] + [outside] * 7, [outside]
    else:
        keys, values, hot = more
        args = (table, q, keys, values, hot)
        specs, out_specs = [small] + [inside] * 4, [inside] * 3
        shapes += [jax.ShapeDtypeStruct(shape, jnp.float32) for shape in state]
    share = 4 if mode else 1
    return pl.pallas_call(
        functools.partial(attend_kernel, mode),
        in_specs=specs,
        out_specs=out_specs,
        out_shape=shapes,
        input_output_aliases={9: 0} if mode else {},
        scratch_shapes=scratch,
        compiler_params=pltpu.CompilerParams(vmem_limit_bytes=60 * MIB),
        cost_estimate=pl.CostEstimate(
            flops=rows * heads * length * length * 128 // share,
            bytes_accessed=8 * rows * width * length,
            transcendentals=rows * length * length // 4 // share,
        ),
    )(*args)


def tables(dec_rows, enc_rows, side):
    rows, whole = dec_rows.shape
    length = whole // 2
    blocks = length // SPAN
    stride, late = (min(size, length) for size in STRIDE)
    numbers = jnp.arange(DOCS, dtype=jnp.int32)[None, :, None]
    bounds = []
    for ids in (enc_rows, dec_rows):
        start = jnp.sum(ids[:, None, :] < numbers, axis=2, dtype=jnp.int32)
        bounds += [start, jnp.concatenate([start[:, 1:], jnp.full((rows, 1), whole, jnp.int32)], axis=1)]
    bounds = jnp.pad(jnp.stack(bounds, axis=1), ((0, 0), (0, 0), (0, LANES - DOCS)))
    mine = lax.dynamic_slice(dec_rows, (0, side * length), (rows, length))
    docs = mine.reshape(rows, blocks, SPAN)
    starts = jnp.concatenate([docs[:, :, 0], dec_rows[:, length : length + 1]], axis=1)
    ends = jnp.concatenate([docs[:, :, -1], dec_rows[:, length - 1 : length]], axis=1)
    before = jnp.sum(enc_rows[:, None, :] < starts[:, :, None], axis=2, dtype=jnp.int32).T
    upto = jnp.sum(enc_rows[:, None, :] <= ends[:, :, None], axis=2, dtype=jnp.int32).T
    ways = jnp.stack([length - before[blocks], upto[blocks] - length])
    ways = -(-jnp.maximum(ways, 0) // PIECE) * PIECE
    most = jnp.max(jnp.sum(ways, axis=1))
    before, upto = before[:blocks], upto[:blocks]
    sent, got = (jnp.where(side == which, ways[0], ways[1]) for which in (0, 1))
    earlier = jnp.arange(rows)[:, None] > jnp.arange(rows)[None, :]
    offset_of = [jnp.sum(jnp.where(earlier, amount[None, :], 0), axis=1) for amount in (sent, got)]
    first = jnp.where(side == 0, length - sent, 0)
    send = jnp.stack([offset_of[0], first, sent])
    base = (offset_of[1] - jnp.where(side == 0, length, length - got))[None, :]
    home = side * length
    near, far = jnp.maximum(before - home, 0), jnp.minimum(upto - home, length)
    low = near // LANES * LANES
    steps = jnp.where(far > near, (far - low + stride - 1) // stride, 0)
    low = jnp.minimum(low, length - steps * stride)
    near = base + jnp.where(side == 0, jnp.maximum(before, length), before)
    far = base + jnp.where(side == 0, upto, jnp.minimum(upto, length))
    start = near // PIECE * PIECE
    more = jnp.where(far > near, (far - start + late - 1) // late, 0)
    known = jnp.concatenate([low, steps, start, more, base, jnp.full((1, rows), side, jnp.int32)], axis=0)
    return send, known, bounds, most


def whole(queries, enc_keys, enc_values, dec_ids, enc_ids):
    group = lax.axis_size("seq")
    half = group // 2
    rows, count, _ = queries.shape
    length = half * count
    side = lax.axis_index("seq") // half
    k, v, ids_all, q_packed = gather(queries, enc_keys, enc_values, dec_ids, enc_ids, group)
    sides = [list(range(half)), list(range(half, group))]

    def cross(block):
        return lax.ppermute(block, "seq", [(i, (i + half) % group) for i in range(group)])

    q = lax.all_to_all(q_packed, "seq", split_axis=0, concat_axis=0, axis_index_groups=sides, tiled=True)
    dec_rows, enc_rows = ids_all.transpose(1, 2, 0, 3).reshape(2, rows, 2 * length)
    send, known, bounds, most = tables(dec_rows, enc_rows, side)
    trip = min(TRIP, length)
    full = rows * length
    room = full * ROOM // 32 // LANES * LANES
    extra = -(-(full - room) // trip) * trip
    more = cross(pack(send, jnp.zeros((1,), jnp.int32), k, v, room))
    q = lax.all_to_all(q_packed, "seq", split_axis=0, concat_axis=0, axis_index_groups=sides, tiled=True)
    keys, values, hot, empty = prepare(known, k, v, bounds, extra)
    most = lax.pmax(most, "dp")
    early, peak, summed = attend(0, known, q, keys, values, hot)
    trips = (jnp.maximum(most - room, 0) + trip - 1) // trip
    more, early = lax.optimization_barrier((more, early))

    def one_trip(index, late):
        piece = cross(pack(send, jnp.full((1,), room + index * trip, jnp.int32), k, v, trip))
        return lax.dynamic_update_slice(late, piece, (index * trip, 0))

    late = lax.fori_loop(0, trips, one_trip, empty)
    sent_late = jnp.stack([trips, jnp.full_like(trips, trip)])
    out = attend(1, known, q, sent_late, bounds, hot, peak, summed, more, late, early)[0]
    return give_back(out, group)


def solution(mesh):
    in_specs = (
        P("dp", "seq", None),
        P("dp", "seq", None),
        P("dp", "seq", None),
        P("dp", "seq"),
        P("dp", "seq"),
    )
    out_specs = P("dp", "seq", None)
    return jax.shard_map(whole, mesh=mesh, in_specs=in_specs, out_specs=out_specs, check_vma=False)
```

```python
import functools

import jax
import jax.numpy as jnp
from jax import lax
from jax.experimental import pallas as pl
from jax.experimental.pallas import tpu as pltpu
from jax.sharding import PartitionSpec as P


HEAD_DIM = 64
TALL = 80
DOCS = 16
LANES = 128
SPAN = 256
STRIDE = (512, 256)
PIECE = 16
TOGETHER = 8
UNROLL = (8, 4)
MIB = 2**20
MASKED = -8192.0
ROOM = 11
TRIP = 512


def peer(me, shift, half):
    base, place = me // half * half, lax.rem(me, half)
    if half & (half - 1):
        return base + lax.rem(place + shift, half)
    bit, flipped = 1, 0
    while bit < half:
        flipped += bit * lax.rem(place // bit + shift // bit, 2)
        bit *= 2
    return base + flipped


def greet(others):
    barrier = pltpu.get_barrier_semaphore()
    for target in others:
        pl.semaphore_signal(barrier, inc=1, device_id={"seq": target}, device_id_type=pl.DeviceIdType.MESH)
    pl.semaphore_wait(barrier, len(others))


def remote(src, dst, send_sem, recv_sem, target):
    return pltpu.make_async_remote_copy(
        src_ref=src,
        dst_ref=dst,
        send_sem=send_sem,
        recv_sem=recv_sem,
        device_id={"seq": target},
        device_id_type=pl.DeviceIdType.MESH,
    )


def gather_kernel(
    group, k_ref, v_ref, dec_ref, enc_ref, q_ref, k_out, v_out, ids_out, q_out, held, ids_held, own_sem, ids_sem, send_sem, recv_sem, ids_send, ids_recv
):
    me = lax.axis_index("seq")
    half = group // 2
    width = k_out.shape[3]
    place = lax.rem(me, half)
    large = ((0, k_ref, k_out), (1, v_ref, v_out))

    def columns(src, target):
        return src.at[:, :, pl.ds(pl.multiple_of(lax.rem(target, half) * width, LANES), width)]

    def heads(shift, slot, src, dst):
        target = peer(me, shift, half)
        at = slot * (half - 1) + shift - 1
        return remote(columns(src, target), dst.at[place], send_sem.at[at], recv_sem.at[at], target)

    def ids(shift):
        at = shift - 1
        return remote(ids_held, ids_out.at[me], ids_send.at[at], ids_recv.at[at], lax.rem(me + shift, group))

    @pl.when(pl.program_id(0) == 0)
    def _():
        own_ids = [
            pltpu.make_async_copy(src, ids_held.at[slot], ids_sem.at[slot]) for slot, src in enumerate((dec_ref, enc_ref))
        ]
        for copy in own_ids:
            copy.start()
        greet([lax.rem(me + shift, group) for shift in range(1, group)])
        for copy in own_ids:
            copy.wait()
        for shift in range(1, half):
            for each in large:
                heads(shift, *each).start()
        for shift in range(1, group):
            ids(shift).start()
        own = [pltpu.make_async_copy(columns(src, me), held.at[slot], own_sem.at[slot]) for slot, src, _ in large]
        own += [pltpu.make_async_copy(ids_held, ids_out.at[me], ids_sem.at[0])]
        for copy in own:
            copy.start()
        for copy in own:
            copy.wait()
        own = [pltpu.make_async_copy(held.at[slot], dst.at[place], own_sem.at[slot]) for slot, _, dst in large]
        for copy in own:
            copy.start()
        for copy in own:
            copy.wait()

    for target in range(half):
        q_out[target, 0] = q_ref[0, :, target * width : (target + 1) * width]

    @pl.when(pl.program_id(0) == pl.num_programs(0) - 1)
    def _():
        for shift in range(1, group):
            ids(shift).wait()
        for each in large:
            for shift in range(1, half):
                heads(shift, *each).wait()


def gather(q, k, v, dec_ids, enc_ids, group):
    rows, count, features = k.shape
    half = group // 2
    width = features // half
    anywhere = pl.BlockSpec(memory_space=pltpu.HBM)
    block = pl.BlockSpec((1, count, features), lambda r: (r, 0, 0))
    packed = pl.BlockSpec((half, 1, count, width), lambda r: (0, r, 0, 0))
    spread = jax.ShapeDtypeStruct((half, rows, count, width), k.dtype)
    every = jax.ShapeDtypeStruct((group, 2, rows, count), dec_ids.dtype)
    dma = pltpu.SemaphoreType.DMA
    return pl.pallas_call(
        functools.partial(gather_kernel, group),
        grid=(rows,),
        in_specs=[anywhere] * 4 + [block],
        out_specs=[anywhere] * 3 + [packed],
        out_shape=[spread, spread, every, spread],
        scratch_shapes=[
            pltpu.VMEM((2, rows, count, width), k.dtype),
            pltpu.VMEM((2, rows, count), dec_ids.dtype),
            dma((2,)),
            dma((2,)),
            dma((2 * (half - 1),)),
            dma((2 * (half - 1),)),
            dma((group - 1,)),
            dma((group - 1,)),
        ],
        compiler_params=pltpu.CompilerParams(collective_id=0, has_side_effects=True),
    )(k, v, dec_ids, enc_ids, q)


def give_back_kernel(group, o_ref, out_ref, held, own_sem, send_sem, recv_sem):
    me = lax.axis_index("seq")
    half = group // 2
    width = o_ref.shape[3]
    place = lax.rem(me, half)
    columns = out_ref.at[:, :, pl.ds(pl.multiple_of(place * width, LANES), width)]

    def transfer(shift):
        target = peer(me, shift, half)
        return remote(o_ref.at[lax.rem(target, half)], columns, send_sem.at[shift - 1], recv_sem.at[shift - 1], target)

    greet([peer(me, shift, half) for shift in range(1, half)])
    for shift in range(1, half):
        transfer(shift).start()
    own = pltpu.make_async_copy(o_ref.at[place], held, own_sem)
    own.start()
    own.wait()
    own = pltpu.make_async_copy(held, columns, own_sem)
    own.start()
    own.wait()
    for shift in range(1, half):
        transfer(shift).wait()


def give_back(o, group):
    half, rows, count, width = o.shape
    return pl.pallas_call(
        functools.partial(give_back_kernel, group),
        in_specs=[pl.BlockSpec(memory_space=pltpu.HBM)],
        out_specs=pl.BlockSpec(memory_space=pltpu.HBM),
        out_shape=jax.ShapeDtypeStruct((rows, count, half * width), o.dtype),
        scratch_shapes=[
            pltpu.VMEM((rows, count, width), o.dtype),
            pltpu.SemaphoreType.DMA,
            pltpu.SemaphoreType.DMA((half - 1,)),
            pltpu.SemaphoreType.DMA((half - 1,)),
        ],
        compiler_params=pltpu.CompilerParams(collective_id=1, has_side_effects=True),
    )(o)


def pack_kernel(table_ref, shift_ref, k_ref, v_ref, o_ref):
    _, rows, count, width = k_ref.shape
    room = o_ref.shape[0]
    o_ref[...] = jnp.zeros(o_ref.shape, o_ref.dtype)

    def one_row(row, carry):
        offset, start, amount = table_ref[0, row] - shift_ref[0], table_ref[1, row], table_ref[2, row]

        def one(index):
            at = start + index * PIECE
            slab, inside = at // count, pl.ds(pl.multiple_of(at % count, PIECE), PIECE)
            into = pl.ds(pl.multiple_of(offset + index * PIECE, PIECE), PIECE)
            o_ref[into, :width] = k_ref[slab, row, inside, :]
            o_ref[into, width:] = v_ref[slab, row, inside, :]

        def move(index, carry):
            one(index)
            return carry

        def several(index, carry):
            for more in range(TOGETHER):
                one(lowest + index * TOGETHER + more)
            return carry

        lowest = jnp.maximum(-offset, 0) // PIECE
        highest = jnp.maximum(jnp.minimum(amount, room - offset) // PIECE, lowest)
        times = (highest - lowest) // TOGETHER
        lax.fori_loop(0, times, several, 0)
        return lax.fori_loop(lowest + times * TOGETHER, highest, move, carry)

    lax.fori_loop(0, rows, one_row, 0)


def pack(table, shift, k, v, room):
    width = k.shape[3]
    small, inside = pl.BlockSpec(memory_space=pltpu.SMEM), pl.BlockSpec(memory_space=pltpu.VMEM)
    return pl.pallas_call(
        pack_kernel,
        in_specs=[small] * 2 + [inside] * 2,
        out_specs=inside,
        out_shape=jax.ShapeDtypeStruct((room, 2 * width), k.dtype),
        compiler_params=pltpu.CompilerParams(vmem_limit_bytes=16 * MIB),
        cost_estimate=pl.CostEstimate(flops=2000000, bytes_accessed=8 * k.size, transcendentals=0),
    )(table, shift, k, v)


def within(low, high, at, amount):
    position = at + lax.broadcasted_iota(jnp.int32, (amount, LANES), 0)
    return (position >= low) & (position < high)


def missing(low, high, at, amount):
    documents = lax.broadcasted_iota(jnp.int32, (amount, LANES), 1)
    return jnp.where(within(low, high, at, amount) | (documents >= DOCS), 0.0, MASKED).astype(jnp.bfloat16)


def tall_values(turned):
    ones = jnp.ones((TALL - HEAD_DIM, turned.shape[1]), turned.dtype)
    return [jnp.concatenate([turned[at : at + HEAD_DIM], ones], axis=0) for at in range(0, turned.shape[0], HEAD_DIM)]


def prepare_kernel(table_ref, k_ref, v_ref, bounds_ref, keys, values, hot, _):
    half, _, count, width = k_ref.shape
    length = half * count
    first = table_ref[table_ref.shape[0] - 1, 0] * length
    bounds = bounds_ref[0]
    keys[0, :, :width] = k_ref[:, 0].reshape(length, width)
    keys[0, :, width:] = missing(bounds[0:1], bounds[1:2], first, length)
    for head, part in enumerate(tall_values(v_ref[:, 0].reshape(length, width).T)):
        values[0, head * TALL : (head + 1) * TALL] = part
    here = jnp.where(within(bounds[2:3], bounds[3:4], first, length), 1.0, 0.0).astype(jnp.bfloat16).T
    hot[0] = here[:DOCS]


def prepare(table, k, v, bounds, extra):
    half, rows, count, width = k.shape
    length = half * count
    row_block = pl.BlockSpec((half, 1, count, width), lambda r, *_: (0, r, 0, 0))
    shapes = [(length, width + LANES), (width // HEAD_DIM * TALL, length), (DOCS, length)]
    return pl.pallas_call(
        prepare_kernel,
        grid_spec=pltpu.PrefetchScalarGridSpec(
            num_scalar_prefetch=1,
            grid=(rows,),
            in_specs=[row_block, row_block, pl.BlockSpec((1, *bounds.shape[1:]), lambda r, *_: (r, 0, 0))],
            out_specs=[pl.BlockSpec((1, *shape), lambda r, *_: (r, 0, 0)) for shape in shapes]
            + [pl.BlockSpec(memory_space=pltpu.HBM)],
        ),
        out_shape=[jax.ShapeDtypeStruct((rows, *shape), k.dtype) for shape in shapes]
        + [jax.ShapeDtypeStruct((extra, 2 * width), k.dtype)],
        cost_estimate=pl.CostEstimate(flops=2000000, bytes_accessed=10 * k.size, transcendentals=0),
    )(table, k, v, bounds)


def attend_kernel(mode, table_ref, *refs):
    if mode:
        trips_ref, bounds_ref, q_from, hot_from, peak_from, sum_from, more_from, late_from, _, o_to, *scratch = refs
        items, even, odd, even_peak, odd_peak, peak_of, sum_of, peak_now, sum_now, q_ref, hot_ref, o_ref, more_ref, sem = scratch
    else:
        q_ref, keys, values, hot_ref, o_ref, peak_of, sum_of, items, even, odd, even_peak, odd_peak = refs
    half, rows, count, width = q_ref.shape
    length = half * count
    heads = width // HEAD_DIM
    _, stride, span = even.shape
    slabs = span // count
    unroll = UNROLL[mode]
    blocks = length // span
    side = table_ref[4 * blocks + 1, 0]

    def entry(row, kind, block):
        return table_ref[kind * blocks + block, row]

    def each_block(do):
        def one(number, carry):
            row, block = number // blocks, number % blocks

            @pl.when(entry(row, 3, block) > 0)
            def _():
                do(number, row, pl.ds(block * slabs, slabs))

            return carry

        lax.fori_loop(0, rows * blocks, one, 0)

    if mode:
        room = more_from.shape[0]
        avail = room + trips_ref[0] * trips_ref[1]

        def move(finish):
            def block(number, row, slab):
                for src, dst in (
                    (q_from.at[slab, row], q_ref.at[slab, row]),
                    (peak_from.at[number], peak_of.at[number]),
                    (sum_from.at[number], sum_of.at[number]),
                ):
                    copy = pltpu.make_async_copy(src, dst, sem)
                    copy.wait() if finish else copy.start()

            for src, dst in ((more_from, more_ref.at[pl.ds(0, room)]), (hot_from, hot_ref)):
                copy = pltpu.make_async_copy(src, dst, sem)
                copy.wait() if finish else copy.start()
            each_block(block)

        move(False)

    def list_block(number, total):
        row, block = number // blocks, number % blocks
        steps = entry(row, 2 * mode + 1, block)
        low = entry(row, 2 * mode, block)
        if mode:
            low = jnp.minimum(low, avail - steps * stride)
        else:

            @pl.when(steps == 0)
            def _():
                peak_of[number] = jnp.full(peak_of.shape[1:], 4 * MASKED, jnp.float32)
                sum_of[number] = jnp.zeros(sum_of.shape[1:], jnp.float32)

        def list_step(index, total):
            items[0, total] = row
            items[1, total] = block
            items[2, total] = low + index * stride
            items[3, total] = (index == 0).astype(jnp.int32)
            return total + 1

        return lax.fori_loop(0, steps, list_step, total)

    total = lax.fori_loop(0, rows * blocks, list_block, jnp.int32(unroll - 1))
    if mode:

        @pl.when(trips_ref[0] > 0)
        def _():
            pltpu.sync_copy(late_from, more_ref.at[pl.ds(room, late_from.shape[0])])

        move(True)

    def score(index, scores, peaks):
        row, block = items[0, index], items[1, index]
        query = q_ref[pl.ds(block * slabs, slabs), row].reshape(span, width).T
        here = hot_ref[row, :, pl.ds(pl.multiple_of(block * span, span), span)]
        owner = lax.broadcasted_iota(jnp.int32, (width, span), 0) // HEAD_DIM
        nothing = jnp.zeros((LANES - DOCS, span), jnp.bfloat16)
        if mode:
            start = pl.multiple_of(items[2, index], PIECE)
            low, high = bounds_ref[row, 0:1], bounds_ref[row, 1:2]
            low = jnp.where(side == 0, jnp.maximum(low, length), low)
            high = jnp.where(side == 0, high, jnp.minimum(high, length))
            miss = missing(low, high, start - table_ref[4 * blocks, row], stride)
            key = jnp.concatenate([more_ref[pl.ds(start, stride), :width], miss], axis=1)
        else:
            start = pl.multiple_of(items[2, index], LANES)
            key = keys[row, pl.ds(start, stride), :]
        for head in range(heads):
            one = jnp.where(owner == head, query, jnp.zeros_like(query))
            result = jnp.dot(key, jnp.concatenate([one, here, nothing], axis=0), preferred_element_type=jnp.float32)
            scores[head] = result
            peaks[head] = jnp.max(result, axis=0, keepdims=True)

    def weigh(index, scores, peaks):
        row, block = items[0, index], items[1, index]
        number, fresh_start = row * blocks + block, items[3, index] == 1
        if mode:
            start = pl.multiple_of(items[2, index], PIECE)
            value = tall_values(more_ref[pl.ds(start, stride), width:].T)
        else:
            start = pl.multiple_of(items[2, index], LANES)
            value = [values[row, head * TALL : (head + 1) * TALL, pl.ds(start, stride)] for head in range(heads)]
        now, at = ((peak_now, sum_now), 0) if mode else ((peak_of, sum_of), number)
        done = []
        for head in range(heads):
            peak, before = (x[at, head] for x in now)
            began = (peak_of[number, head], sum_of[number, head]) if mode else (4 * MASKED, 0.0)
            peak, before = jnp.where(fresh_start, began[0], peak), jnp.where(fresh_start, began[1], before)
            fresh = jnp.maximum(peak, peaks[head])
            now[0][at, head] = fresh
            expos = jnp.exp(scores[head] - fresh).astype(jnp.bfloat16)
            summed = before * jnp.exp(peak - fresh) + jnp.dot(value[head], expos, preferred_element_type=jnp.float32)
            now[1][at, head] = summed
            done.append(summed[:HEAD_DIM] / summed[HEAD_DIM : HEAD_DIM + 1])
        whole = jnp.concatenate(done, axis=0).T.astype(jnp.bfloat16)
        o_ref[pl.ds(block * slabs, slabs), row] = whole.reshape(slabs, count, width)

    @pl.when(total >= unroll)
    def _():
        begin = total % unroll
        for spare in range(unroll - 1):
            for field in range(4):
                items[field, spare] = items[field, unroll - 1]
        score(begin, even, even_peak)

        def several(index, carry):
            at = begin + unroll * index
            buffers = ((even, even_peak), (odd, odd_peak))
            for ahead in range(unroll):
                score(jnp.minimum(at + ahead + 1, total - 1), *buffers[(ahead + 1) % 2])
                weigh(at + ahead, *buffers[ahead % 2])
            return carry

        lax.fori_loop(0, (total - begin) // unroll, several, 0)

    if mode:

        def put(finish):
            def block(number, row, slab):
                copy = pltpu.make_async_copy(o_ref.at[slab, row], o_to.at[slab, row], sem)
                copy.wait() if finish else copy.start()

            each_block(block)

        put(False)
        put(True)


def attend(mode, table, q, *more):
    half, rows, count, width = q.shape
    length = half * count
    heads = width // HEAD_DIM
    span = max(SPAN, count)
    stride = min(STRIDE[mode], length)
    small = pl.BlockSpec(memory_space=pltpu.SMEM)
    inside = pl.BlockSpec(memory_space=pltpu.VMEM)
    outside = pl.BlockSpec(memory_space=pltpu.HBM)
    numbers = rows * (length // span)
    state = [(numbers, heads, 1, span), (numbers, heads, TALL, span)]
    scratch = [
        pltpu.SMEM((4, numbers * (2 * length // stride + 1) + UNROLL[mode]), jnp.int32),
        pltpu.VMEM((heads, stride, span), jnp.float32),
        pltpu.VMEM((heads, stride, span), jnp.float32),
        pltpu.VMEM((heads, 1, span), jnp.float32),
        pltpu.VMEM((heads, 1, span), jnp.float32),
    ]
    shapes = [jax.ShapeDtypeStruct(q.shape, q.dtype)]
    if mode:
        trips, bounds, hot, peak, summed, cross, late, early = more
        scratch += [pltpu.VMEM(shape, jnp.float32) for shape in state + [(1, *shape[1:]) for shape in state]]
        scratch += [
            pltpu.VMEM(q.shape, q.dtype),
            pltpu.VMEM(hot.shape, q.dtype),
            pltpu.VMEM(q.shape, q.dtype),
            pltpu.VMEM((cross.shape[0] + late.shape[0], 2 * width), q.dtype),
            pltpu.SemaphoreType.DMA,
        ]
        args = (table, trips, bounds, q, hot, peak, summed, cross, late, early)
        specs, out_specs = [small] * 2 + [inside] + [outside] * 7, [outside]
    else:
        keys, values, hot = more
        args = (table, q, keys, values, hot)
        specs, out_specs = [small] + [inside] * 4, [inside] * 3
        shapes += [jax.ShapeDtypeStruct(shape, jnp.float32) for shape in state]
    share = 4 if mode else 1
    return pl.pallas_call(
        functools.partial(attend_kernel, mode),
        in_specs=specs,
        out_specs=out_specs,
        out_shape=shapes,
        input_output_aliases={9: 0} if mode else {},
        scratch_shapes=scratch,
        compiler_params=pltpu.CompilerParams(vmem_limit_bytes=60 * MIB),
        cost_estimate=pl.CostEstimate(
            flops=rows * heads * length * length * 128 // share,
            bytes_accessed=8 * rows * width * length,
            transcendentals=rows * length * length // 4 // share,
        ),
    )(*args)


def tables(dec_rows, enc_rows, side):
    rows, whole = dec_rows.shape
    length = whole // 2
    blocks = length // SPAN
    stride, late = (min(size, length) for size in STRIDE)
    numbers = jnp.arange(DOCS, dtype=jnp.int32)[None, :, None]
    bounds = []
    for ids in (enc_rows, dec_rows):
        start = jnp.sum(ids[:, None, :] < numbers, axis=2, dtype=jnp.int32)
        bounds += [start, jnp.concatenate([start[:, 1:], jnp.full((rows, 1), whole, jnp.int32)], axis=1)]
    bounds = jnp.pad(jnp.stack(bounds, axis=1), ((0, 0), (0, 0), (0, LANES - DOCS)))
    mine = lax.dynamic_slice(dec_rows, (0, side * length), (rows, length))
    docs = mine.reshape(rows, blocks, SPAN)
    starts = jnp.concatenate([docs[:, :, 0], dec_rows[:, length : length + 1]], axis=1)
    ends = jnp.concatenate([docs[:, :, -1], dec_rows[:, length - 1 : length]], axis=1)
    before = jnp.sum(enc_rows[:, None, :] < starts[:, :, None], axis=2, dtype=jnp.int32).T
    upto = jnp.sum(enc_rows[:, None, :] <= ends[:, :, None], axis=2, dtype=jnp.int32).T
    ways = jnp.stack([length - before[blocks], upto[blocks] - length])
    ways = -(-jnp.maximum(ways, 0) // PIECE) * PIECE
    most = jnp.max(jnp.sum(ways, axis=1))
    before, upto = before[:blocks], upto[:blocks]
    sent, got = (jnp.where(side == which, ways[0], ways[1]) for which in (0, 1))
    earlier = jnp.arange(rows)[:, None] > jnp.arange(rows)[None, :]
    offset_of = [jnp.sum(jnp.where(earlier, amount[None, :], 0), axis=1) for amount in (sent, got)]
    first = jnp.where(side == 0, length - sent, 0)
    send = jnp.stack([offset_of[0], first, sent])
    base = (offset_of[1] - jnp.where(side == 0, length, length - got))[None, :]
    home = side * length
    near, far = jnp.maximum(before - home, 0), jnp.minimum(upto - home, length)
    low = near // LANES * LANES
    steps = jnp.where(far > near, (far - low + stride - 1) // stride, 0)
    low = jnp.minimum(low, length - steps * stride)
    near = base + jnp.where(side == 0, jnp.maximum(before, length), before)
    far = base + jnp.where(side == 0, upto, jnp.minimum(upto, length))
    start = near // PIECE * PIECE
    more = jnp.where(far > near, (far - start + late - 1) // late, 0)
    known = jnp.concatenate([low, steps, start, more, base, jnp.full((1, rows), side, jnp.int32)], axis=0)
    return send, known, bounds, most


def whole(queries, enc_keys, enc_values, dec_ids, enc_ids):
    group = lax.axis_size("seq")
    half = group // 2
    rows, count, _ = queries.shape
    length = half * count
    side = lax.axis_index("seq") // half
    k, v, ids_all, q_packed = gather(queries, enc_keys, enc_values, dec_ids, enc_ids, group)
    sides = [list(range(half)), list(range(half, group))]

    def cross(block):
        return lax.ppermute(block, "seq", [(i, (i + half) % group) for i in range(group)])

    q = lax.all_to_all(q_packed, "seq", split_axis=0, concat_axis=0, axis_index_groups=sides, tiled=True)
    dec_rows, enc_rows = ids_all.transpose(1, 2, 0, 3).reshape(2, rows, 2 * length)
    send, known, bounds, most = tables(dec_rows, enc_rows, side)
    trip = min(TRIP, length)
    full = rows * length
    room = full * ROOM // 32 // LANES * LANES
    extra = -(-(full - room) // trip) * trip
    more = cross(pack(send, jnp.zeros((1,), jnp.int32), k, v, room))
    q = lax.all_to_all(q_packed, "seq", split_axis=0, concat_axis=0, axis_index_groups=sides, tiled=True)
    keys, values, hot, empty = prepare(known, k, v, bounds, extra)
    most = lax.pmax(most, "dp")
    early, peak, summed = attend(0, known, q, keys, values, hot)
    trips = (jnp.maximum(most - room, 0) + trip - 1) // trip
    more, early = lax.optimization_barrier((more, early))

    def one_trip(index, late):
        piece = cross(pack(send, jnp.full((1,), room + index * trip, jnp.int32), k, v, trip))
        return lax.dynamic_update_slice(late, piece, (index * trip, 0))

    late = lax.fori_loop(0, trips, one_trip, empty)
    sent_late = jnp.stack([trips, jnp.full_like(trips, trip)])
    out = attend(1, known, q, sent_late, bounds, hot, peak, summed, more, late, early)[0]
    return give_back(out, group)


def solution(mesh):
    in_specs = (
        P("dp", "seq", None),
        P("dp", "seq", None),
        P("dp", "seq", None),
        P("dp", "seq"),
        P("dp", "seq"),
    )
    out_specs = P("dp", "seq", None)
    return jax.shard_map(whole, mesh=mesh, in_specs=in_specs, out_specs=out_specs, check_vma=False)
```

```python
import functools

import jax
import jax.numpy as jnp
from jax import lax
from jax.experimental import pallas as pl
from jax.experimental.pallas import tpu as pltpu
from jax.sharding import PartitionSpec as P


HEAD_DIM = 64
TALL = 80
DOCS = 16
LANES = 128
SPAN = 256
STRIDE = (512, 256)
PIECE = 16
TOGETHER = 8
UNROLL = (8, 4)
MIB = 2**20
MASKED = -8192.0
ROOM = 11
TRIP = 512


def peer(me, shift, half):
    base, place = me // half * half, me % half
    if half & (half - 1):
        return base + (place + shift) % half
    bit, flipped = 1, 0
    while bit < half:
        flipped += bit * ((place // bit + shift // bit) % 2)
        bit *= 2
    return base + flipped


def origin(me, shift, half):
    return peer(me, (half - shift) % half if half & (half - 1) else shift, half)


def greet(others):
    barrier = pltpu.get_barrier_semaphore()
    for target in others:
        pl.semaphore_signal(barrier, inc=1, device_id={"seq": target}, device_id_type=pl.DeviceIdType.MESH)
    pl.semaphore_wait(barrier, len(others))


def remote(src, dst, send_sem, recv_sem, target):
    return pltpu.make_async_remote_copy(
        src_ref=src,
        dst_ref=dst,
        send_sem=send_sem,
        recv_sem=recv_sem,
        device_id={"seq": target},
        device_id_type=pl.DeviceIdType.MESH,
    )


def gather_kernel(
    group, k_ref, v_ref, dec_ref, enc_ref, q_ref, k_out, v_out, ids_out, *rest
):
    me = lax.axis_index("seq")
    half = group // 2
    q_outs, rest = rest[:half], rest[half:]
    held, ids_held, own_sem, ids_sem, send_sem, recv_sem, ids_send, ids_recv = rest
    width = k_out.shape[3]
    place = lax.rem(me, half)
    large = ((0, k_ref, k_out), (1, v_ref, v_out))

    def columns(src, target):
        return src.at[:, :, pl.ds(pl.multiple_of(lax.rem(target, half) * width, LANES), width)]

    def heads(shift, slot, src, dst):
        target = peer(me, shift, half)
        at = slot * (half - 1) + shift - 1
        return remote(columns(src, target), dst.at[place], send_sem.at[at], recv_sem.at[at], target)

    def ids(shift):
        at = shift - 1
        return remote(ids_held, ids_out.at[me], ids_send.at[at], ids_recv.at[at], lax.rem(me + shift, group))

    @pl.when(pl.program_id(0) == 0)
    def _():
        own_ids = [
            pltpu.make_async_copy(src, ids_held.at[slot], ids_sem.at[slot]) for slot, src in enumerate((dec_ref, enc_ref))
        ]
        for copy in own_ids:
            copy.start()
        greet([lax.rem(me + shift, group) for shift in range(1, group)])
        for copy in own_ids:
            copy.wait()
        for shift in range(1, half):
            for each in large:
                heads(shift, *each).start()
        for shift in range(1, group):
            ids(shift).start()
        own = [pltpu.make_async_copy(columns(src, me), held.at[slot], own_sem.at[slot]) for slot, src, _ in large]
        own += [pltpu.make_async_copy(ids_held, ids_out.at[me], ids_sem.at[0])]
        for copy in own:
            copy.start()
        for copy in own:
            copy.wait()
        own = [pltpu.make_async_copy(held.at[slot], dst.at[place], own_sem.at[slot]) for slot, _, dst in large]
        for copy in own:
            copy.start()
        for copy in own:
            copy.wait()

    for shift, q_out in enumerate(q_outs):
        target = lax.rem(peer(me, shift, half), half)
        q_out[0] = q_ref[0, :, pl.ds(pl.multiple_of(target * width, LANES), width)]

    @pl.when(pl.program_id(0) == pl.num_programs(0) - 1)
    def _():
        for shift in range(1, group):
            ids(shift).wait()
        for each in large:
            for shift in range(1, half):
                heads(shift, *each).wait()


def gather(q, k, v, dec_ids, enc_ids, group):
    rows, count, features = k.shape
    half = group // 2
    width = features // half
    anywhere = pl.BlockSpec(memory_space=pltpu.HBM)
    block = pl.BlockSpec((1, count, features), lambda r: (r, 0, 0))
    packed = pl.BlockSpec((1, count, width), lambda r: (r, 0, 0))
    spread = jax.ShapeDtypeStruct((half, rows, count, width), k.dtype)
    every = jax.ShapeDtypeStruct((group, 2, rows, count), dec_ids.dtype)
    dma = pltpu.SemaphoreType.DMA
    return pl.pallas_call(
        functools.partial(gather_kernel, group),
        grid=(rows,),
        in_specs=[anywhere] * 4 + [block],
        out_specs=[anywhere] * 3 + [packed] * half,
        out_shape=[spread, spread, every] + [jax.ShapeDtypeStruct((rows, count, width), q.dtype)] * half,
        scratch_shapes=[
            pltpu.VMEM((2, rows, count, width), k.dtype),
            pltpu.VMEM((2, rows, count), dec_ids.dtype),
            dma((2,)),
            dma((2,)),
            dma((2 * (half - 1),)),
            dma((2 * (half - 1),)),
            dma((group - 1,)),
            dma((group - 1,)),
        ],
        compiler_params=pltpu.CompilerParams(collective_id=0, has_side_effects=True),
    )(k, v, dec_ids, enc_ids, q)


def give_back_kernel(group, o_ref, out_ref, held, own_sem, send_sem, recv_sem):
    me = lax.axis_index("seq")
    half = group // 2
    width = o_ref.shape[3]
    place = lax.rem(me, half)
    columns = out_ref.at[:, :, pl.ds(pl.multiple_of(place * width, LANES), width)]

    def transfer(shift):
        target = peer(me, shift, half)
        return remote(o_ref.at[lax.rem(target, half)], columns, send_sem.at[shift - 1], recv_sem.at[shift - 1], target)

    greet([peer(me, shift, half) for shift in range(1, half)])
    for shift in range(1, half):
        transfer(shift).start()
    own = pltpu.make_async_copy(o_ref.at[place], held, own_sem)
    own.start()
    own.wait()
    own = pltpu.make_async_copy(held, columns, own_sem)
    own.start()
    own.wait()
    for shift in range(1, half):
        transfer(shift).wait()


def give_back(o, group):
    half, rows, count, width = o.shape
    return pl.pallas_call(
        functools.partial(give_back_kernel, group),
        in_specs=[pl.BlockSpec(memory_space=pltpu.HBM)],
        out_specs=pl.BlockSpec(memory_space=pltpu.HBM),
        out_shape=jax.ShapeDtypeStruct((rows, count, half * width), o.dtype),
        scratch_shapes=[
            pltpu.VMEM((rows, count, width), o.dtype),
            pltpu.SemaphoreType.DMA,
            pltpu.SemaphoreType.DMA((half - 1,)),
            pltpu.SemaphoreType.DMA((half - 1,)),
        ],
        compiler_params=pltpu.CompilerParams(collective_id=1, has_side_effects=True),
    )(o)


def pack_kernel(table_ref, shift_ref, k_ref, v_ref, o_ref):
    _, rows, count, width = k_ref.shape
    room = o_ref.shape[0]
    o_ref[...] = jnp.zeros(o_ref.shape, o_ref.dtype)

    def one_row(row, carry):
        offset, start, amount = table_ref[0, row] - shift_ref[0], table_ref[1, row], table_ref[2, row]

        def one(index):
            at = start + index * PIECE
            slab, inside = at // count, pl.ds(pl.multiple_of(at % count, PIECE), PIECE)
            into = pl.ds(pl.multiple_of(offset + index * PIECE, PIECE), PIECE)
            o_ref[into, :width] = k_ref[slab, row, inside, :]
            o_ref[into, width:] = v_ref[slab, row, inside, :]

        def move(index, carry):
            one(index)
            return carry

        def several(index, carry):
            for more in range(TOGETHER):
                one(lowest + index * TOGETHER + more)
            return carry

        lowest = jnp.maximum(-offset, 0) // PIECE
        highest = jnp.maximum(jnp.minimum(amount, room - offset) // PIECE, lowest)
        times = (highest - lowest) // TOGETHER
        lax.fori_loop(0, times, several, 0)
        return lax.fori_loop(lowest + times * TOGETHER, highest, move, carry)

    lax.fori_loop(0, rows, one_row, 0)


def pack(table, shift, k, v, room):
    width = k.shape[3]
    small, inside = pl.BlockSpec(memory_space=pltpu.SMEM), pl.BlockSpec(memory_space=pltpu.VMEM)
    return pl.pallas_call(
        pack_kernel,
        in_specs=[small] * 2 + [inside] * 2,
        out_specs=inside,
        out_shape=jax.ShapeDtypeStruct((room, 2 * width), k.dtype),
        compiler_params=pltpu.CompilerParams(vmem_limit_bytes=16 * MIB),
        cost_estimate=pl.CostEstimate(flops=2000000, bytes_accessed=8 * k.size, transcendentals=0),
    )(table, shift, k, v)


def within(low, high, at, amount):
    position = at + lax.broadcasted_iota(jnp.int32, (amount, LANES), 0)
    return (position >= low) & (position < high)


def missing(low, high, at, amount):
    documents = lax.broadcasted_iota(jnp.int32, (amount, LANES), 1)
    return jnp.where(within(low, high, at, amount) | (documents >= DOCS), 0.0, MASKED).astype(jnp.bfloat16)


def tall_values(turned):
    ones = jnp.ones((TALL - HEAD_DIM, turned.shape[1]), turned.dtype)
    return [jnp.concatenate([turned[at : at + HEAD_DIM], ones], axis=0) for at in range(0, turned.shape[0], HEAD_DIM)]


def prepare_kernel(table_ref, k_ref, v_ref, bounds_ref, keys, values, hot, _):
    half, _, count, width = k_ref.shape
    length = half * count
    first = table_ref[table_ref.shape[0] - 1, 0] * length
    bounds = bounds_ref[0]
    keys[0, :, :width] = k_ref[:, 0].reshape(length, width)
    keys[0, :, width:] = missing(bounds[0:1], bounds[1:2], first, length)
    for head, part in enumerate(tall_values(v_ref[:, 0].reshape(length, width).T)):
        values[0, head * TALL : (head + 1) * TALL] = part
    here = jnp.where(within(bounds[2:3], bounds[3:4], first, length), 1.0, 0.0).astype(jnp.bfloat16).T
    hot[0] = here[:DOCS]


def prepare(table, k, v, bounds, extra):
    half, rows, count, width = k.shape
    length = half * count
    row_block = pl.BlockSpec((half, 1, count, width), lambda r, *_: (0, r, 0, 0))
    shapes = [(length, width + LANES), (width // HEAD_DIM * TALL, length), (DOCS, length)]
    return pl.pallas_call(
        prepare_kernel,
        grid_spec=pltpu.PrefetchScalarGridSpec(
            num_scalar_prefetch=1,
            grid=(rows,),
            in_specs=[row_block, row_block, pl.BlockSpec((1, *bounds.shape[1:]), lambda r, *_: (r, 0, 0))],
            out_specs=[pl.BlockSpec((1, *shape), lambda r, *_: (r, 0, 0)) for shape in shapes]
            + [pl.BlockSpec(memory_space=pltpu.HBM)],
        ),
        out_shape=[jax.ShapeDtypeStruct((rows, *shape), k.dtype) for shape in shapes]
        + [jax.ShapeDtypeStruct((extra, 2 * width), k.dtype)],
        cost_estimate=pl.CostEstimate(flops=2000000, bytes_accessed=10 * k.size, transcendentals=0),
    )(table, k, v, bounds)


def attend_kernel(mode, table_ref, *refs):
    if mode:
        trips_ref, bounds_ref, q_from, hot_from, peak_from, sum_from, more_from, late_from, _, o_to, *scratch = refs
        items, even, odd, even_peak, odd_peak, peak_of, sum_of, peak_now, sum_now, q_ref, hot_ref, o_ref, more_ref, sem = scratch
    else:
        parts = refs[: len(refs) - 12]
        keys, values, hot_ref, o_ref, q_ref, peak_of, sum_of, items, even, odd, even_peak, odd_peak = refs[len(parts) :]
        place = lax.axis_index("seq")
        for shift, part in enumerate(parts):
            q_ref[lax.rem(origin(place, shift, len(parts)), len(parts))] = part[...]
    half, rows, count, width = q_ref.shape
    length = half * count
    heads = width // HEAD_DIM
    _, stride, span = even.shape
    slabs = span // count
    unroll = UNROLL[mode]
    blocks = length // span
    side = table_ref[4 * blocks + 1, 0]

    def entry(row, kind, block):
        return table_ref[kind * blocks + block, row]

    def each_block(do):
        def one(number, carry):
            row, block = number // blocks, number % blocks

            @pl.when(entry(row, 3, block) > 0)
            def _():
                do(number, row, pl.ds(block * slabs, slabs))

            return carry

        lax.fori_loop(0, rows * blocks, one, 0)

    if mode:
        room = more_from.shape[0]
        avail = room + trips_ref[0] * trips_ref[1]

        def move(finish):
            def block(number, row, slab):
                for src, dst in (
                    (q_from.at[slab, row], q_ref.at[slab, row]),
                    (peak_from.at[number], peak_of.at[number]),
                    (sum_from.at[number], sum_of.at[number]),
                ):
                    copy = pltpu.make_async_copy(src, dst, sem)
                    copy.wait() if finish else copy.start()

            for src, dst in ((more_from, more_ref.at[pl.ds(0, room)]), (hot_from, hot_ref)):
                copy = pltpu.make_async_copy(src, dst, sem)
                copy.wait() if finish else copy.start()
            each_block(block)

        move(False)

    def list_block(number, total):
        row, block = number // blocks, number % blocks
        steps = entry(row, 2 * mode + 1, block)
        low = entry(row, 2 * mode, block)
        if mode:
            low = jnp.minimum(low, avail - steps * stride)
        else:

            @pl.when(steps == 0)
            def _():
                peak_of[number] = jnp.full(peak_of.shape[1:], 4 * MASKED, jnp.float32)
                sum_of[number] = jnp.zeros(sum_of.shape[1:], jnp.float32)

        def list_step(index, total):
            items[0, total] = row
            items[1, total] = block
            items[2, total] = low + index * stride
            items[3, total] = (index == 0).astype(jnp.int32)
            return total + 1

        return lax.fori_loop(0, steps, list_step, total)

    total = lax.fori_loop(0, rows * blocks, list_block, jnp.int32(unroll - 1))
    if mode:

        @pl.when(trips_ref[0] > 0)
        def _():
            pltpu.sync_copy(late_from, more_ref.at[pl.ds(room, late_from.shape[0])])

        move(True)

    def score(index, scores, peaks):
        row, block = items[0, index], items[1, index]
        query = q_ref[pl.ds(block * slabs, slabs), row].reshape(span, width).T
        here = hot_ref[row, :, pl.ds(pl.multiple_of(block * span, span), span)]
        owner = lax.broadcasted_iota(jnp.int32, (width, span), 0) // HEAD_DIM
        nothing = jnp.zeros((LANES - DOCS, span), jnp.bfloat16)
        if mode:
            start = pl.multiple_of(items[2, index], PIECE)
            low, high = bounds_ref[row, 0:1], bounds_ref[row, 1:2]
            low = jnp.where(side == 0, jnp.maximum(low, length), low)
            high = jnp.where(side == 0, high, jnp.minimum(high, length))
            miss = missing(low, high, start - table_ref[4 * blocks, row], stride)
            key = jnp.concatenate([more_ref[pl.ds(start, stride), :width], miss], axis=1)
        else:
            start = pl.multiple_of(items[2, index], LANES)
            key = keys[row, pl.ds(start, stride), :]
        for head in range(heads):
            one = jnp.where(owner == head, query, jnp.zeros_like(query))
            result = jnp.dot(key, jnp.concatenate([one, here, nothing], axis=0), preferred_element_type=jnp.float32)
            scores[head] = result
            peaks[head] = jnp.max(result, axis=0, keepdims=True)

    def weigh(index, scores, peaks):
        row, block = items[0, index], items[1, index]
        number, fresh_start = row * blocks + block, items[3, index] == 1
        if mode:
            start = pl.multiple_of(items[2, index], PIECE)
            value = tall_values(more_ref[pl.ds(start, stride), width:].T)
        else:
            start = pl.multiple_of(items[2, index], LANES)
            value = [values[row, head * TALL : (head + 1) * TALL, pl.ds(start, stride)] for head in range(heads)]
        now, at = ((peak_now, sum_now), 0) if mode else ((peak_of, sum_of), number)
        done = []
        for head in range(heads):
            peak, before = (x[at, head] for x in now)
            began = (peak_of[number, head], sum_of[number, head]) if mode else (4 * MASKED, 0.0)
            peak, before = jnp.where(fresh_start, began[0], peak), jnp.where(fresh_start, began[1], before)
            fresh = jnp.maximum(peak, peaks[head])
            now[0][at, head] = fresh
            expos = jnp.exp(scores[head] - fresh).astype(jnp.bfloat16)
            summed = before * jnp.exp(peak - fresh) + jnp.dot(value[head], expos, preferred_element_type=jnp.float32)
            now[1][at, head] = summed
            done.append(summed[:HEAD_DIM] / summed[HEAD_DIM : HEAD_DIM + 1])
        whole = jnp.concatenate(done, axis=0).T.astype(jnp.bfloat16)
        o_ref[pl.ds(block * slabs, slabs), row] = whole.reshape(slabs, count, width)

    @pl.when(total >= unroll)
    def _():
        begin = total % unroll
        for spare in range(unroll - 1):
            for field in range(4):
                items[field, spare] = items[field, unroll - 1]
        score(begin, even, even_peak)

        def several(index, carry):
            at = begin + unroll * index
            buffers = ((even, even_peak), (odd, odd_peak))
            for ahead in range(unroll):
                score(jnp.minimum(at + ahead + 1, total - 1), *buffers[(ahead + 1) % 2])
                weigh(at + ahead, *buffers[ahead % 2])
            return carry

        lax.fori_loop(0, (total - begin) // unroll, several, 0)

    if mode:

        def put(finish):
            def block(number, row, slab):
                copy = pltpu.make_async_copy(o_ref.at[slab, row], o_to.at[slab, row], sem)
                copy.wait() if finish else copy.start()

            each_block(block)

        put(False)
        put(True)


def attend(mode, table, q, *more):
    parts = () if mode else q
    if parts:
        q = jax.ShapeDtypeStruct((len(parts), *parts[0].shape), parts[0].dtype)
    half, rows, count, width = q.shape
    length = half * count
    heads = width // HEAD_DIM
    span = max(SPAN, count)
    stride = min(STRIDE[mode], length)
    small = pl.BlockSpec(memory_space=pltpu.SMEM)
    inside = pl.BlockSpec(memory_space=pltpu.VMEM)
    outside = pl.BlockSpec(memory_space=pltpu.HBM)
    numbers = rows * (length // span)
    state = [(numbers, heads, 1, span), (numbers, heads, TALL, span)]
    scratch = [
        pltpu.SMEM((4, numbers * (2 * length // stride + 1) + UNROLL[mode]), jnp.int32),
        pltpu.VMEM((heads, stride, span), jnp.float32),
        pltpu.VMEM((heads, stride, span), jnp.float32),
        pltpu.VMEM((heads, 1, span), jnp.float32),
        pltpu.VMEM((heads, 1, span), jnp.float32),
    ]
    shapes = [jax.ShapeDtypeStruct(q.shape, q.dtype)]
    if mode:
        trips, bounds, hot, peak, summed, cross, late, early = more
        scratch += [pltpu.VMEM(shape, jnp.float32) for shape in state + [(1, *shape[1:]) for shape in state]]
        scratch += [
            pltpu.VMEM(q.shape, q.dtype),
            pltpu.VMEM(hot.shape, q.dtype),
            pltpu.VMEM(q.shape, q.dtype),
            pltpu.VMEM((cross.shape[0] + late.shape[0], 2 * width), q.dtype),
            pltpu.SemaphoreType.DMA,
        ]
        args = (table, trips, bounds, q, hot, peak, summed, cross, late, early)
        specs, out_specs = [small] * 2 + [inside] + [outside] * 7, [outside]
    else:
        keys, values, hot = more
        args = (table, *parts, keys, values, hot)
        specs, out_specs = [small] + [inside] * (half + 3), [inside] * 4
        shapes += [jax.ShapeDtypeStruct(q.shape, q.dtype)]
        shapes += [jax.ShapeDtypeStruct(shape, jnp.float32) for shape in state]
    share = 4 if mode else 1
    return pl.pallas_call(
        functools.partial(attend_kernel, mode),
        in_specs=specs,
        out_specs=out_specs,
        out_shape=shapes,
        input_output_aliases={9: 0} if mode else {},
        scratch_shapes=scratch,
        compiler_params=pltpu.CompilerParams(vmem_limit_bytes=60 * MIB),
        cost_estimate=pl.CostEstimate(
            flops=rows * heads * length * length * 128 // share,
            bytes_accessed=8 * rows * width * length,
            transcendentals=rows * length * length // 4 // share,
        ),
    )(*args)


def tables(dec_rows, enc_rows, side):
    rows, whole = dec_rows.shape
    length = whole // 2
    blocks = length // SPAN
    stride, late = (min(size, length) for size in STRIDE)
    numbers = jnp.arange(DOCS, dtype=jnp.int32)[None, :, None]
    bounds = []
    for ids in (enc_rows, dec_rows):
        start = jnp.sum(ids[:, None, :] < numbers, axis=2, dtype=jnp.int32)
        bounds += [start, jnp.concatenate([start[:, 1:], jnp.full((rows, 1), whole, jnp.int32)], axis=1)]
    bounds = jnp.pad(jnp.stack(bounds, axis=1), ((0, 0), (0, 0), (0, LANES - DOCS)))
    mine = lax.dynamic_slice(dec_rows, (0, side * length), (rows, length))
    docs = mine.reshape(rows, blocks, SPAN)
    starts = jnp.concatenate([docs[:, :, 0], dec_rows[:, length : length + 1]], axis=1)
    ends = jnp.concatenate([docs[:, :, -1], dec_rows[:, length - 1 : length]], axis=1)
    before = jnp.sum(enc_rows[:, None, :] < starts[:, :, None], axis=2, dtype=jnp.int32).T
    upto = jnp.sum(enc_rows[:, None, :] <= ends[:, :, None], axis=2, dtype=jnp.int32).T
    ways = jnp.stack([length - before[blocks], upto[blocks] - length])
    ways = -(-jnp.maximum(ways, 0) // PIECE) * PIECE
    most = jnp.max(jnp.sum(ways, axis=1))
    before, upto = before[:blocks], upto[:blocks]
    sent, got = (jnp.where(side == which, ways[0], ways[1]) for which in (0, 1))
    earlier = jnp.arange(rows)[:, None] > jnp.arange(rows)[None, :]
    offset_of = [jnp.sum(jnp.where(earlier, amount[None, :], 0), axis=1) for amount in (sent, got)]
    first = jnp.where(side == 0, length - sent, 0)
    send = jnp.stack([offset_of[0], first, sent])
    base = (offset_of[1] - jnp.where(side == 0, length, length - got))[None, :]
    home = side * length
    near, far = jnp.maximum(before - home, 0), jnp.minimum(upto - home, length)
    low = near // LANES * LANES
    steps = jnp.where(far > near, (far - low + stride - 1) // stride, 0)
    low = jnp.minimum(low, length - steps * stride)
    near = base + jnp.where(side == 0, jnp.maximum(before, length), before)
    far = base + jnp.where(side == 0, upto, jnp.minimum(upto, length))
    start = near // PIECE * PIECE
    more = jnp.where(far > near, (far - start + late - 1) // late, 0)
    known = jnp.concatenate([low, steps, start, more, base, jnp.full((1, rows), side, jnp.int32)], axis=0)
    return send, known, bounds, most


def whole(queries, enc_keys, enc_values, dec_ids, enc_ids):
    group = lax.axis_size("seq")
    half = group // 2
    rows, count, _ = queries.shape
    length = half * count
    side = lax.axis_index("seq") // half
    k, v, ids_all, *queries = gather(queries, enc_keys, enc_values, dec_ids, enc_ids, group)
    moves = [[(i, int(peer(i, shift, half))) for i in range(group)] for shift in range(1, half)]

    def cross(block):
        return lax.ppermute(block, "seq", [(i, (i + half) % group) for i in range(group)])

    parts = queries[:1] + [lax.ppermute(part, "seq", move) for part, move in zip(queries[1:], moves)]
    dec_rows, enc_rows = ids_all.transpose(1, 2, 0, 3).reshape(2, rows, 2 * length)
    send, known, bounds, most = tables(dec_rows, enc_rows, side)
    trip = min(TRIP, length)
    full = rows * length
    room = full * ROOM // 32 // LANES * LANES
    extra = -(-(full - room) // trip) * trip
    more = cross(pack(send, jnp.zeros((1,), jnp.int32), k, v, room))
    parts = queries[:1] + [lax.ppermute(part, "seq", move) for part, move in zip(queries[1:], moves)]
    keys, values, hot, empty = prepare(known, k, v, bounds, extra)
    most = lax.pmax(most, "dp")
    early, q, peak, summed = attend(0, known, parts, keys, values, hot)
    trips = (jnp.maximum(most - room, 0) + trip - 1) // trip
    more, early = lax.optimization_barrier((more, early))

    def one_trip(index, late):
        piece = cross(pack(send, jnp.full((1,), room + index * trip, jnp.int32), k, v, trip))
        return lax.dynamic_update_slice(late, piece, (index * trip, 0))

    late = lax.fori_loop(0, trips, one_trip, empty)
    sent_late = jnp.stack([trips, jnp.full_like(trips, trip)])
    out = attend(1, known, q, sent_late, bounds, hot, peak, summed, more, late, early)[0]
    return give_back(out, group)


def solution(mesh):
    in_specs = (
        P("dp", "seq", None),
        P("dp", "seq", None),
        P("dp", "seq", None),
        P("dp", "seq"),
        P("dp", "seq"),
    )
    out_specs = P("dp", "seq", None)
    return jax.shard_map(whole, mesh=mesh, in_specs=in_specs, out_specs=out_specs, check_vma=False)
```
